16 devices in a mesh: dp: 2 (over z), fsdp: 8 (over y, x, core).
Axes of the slice: x: 2, y: 2, z: 2, core: 2. Of those that a mesh axis runs over, the one named last changes fastest.
Arguments:
- tokens: int32 [256, 256], P(('dp', 'fsdp'))
- grad_y: bfloat16 [256, 256, 1024], P(('dp', 'fsdp'))
- embedding: bfloat16 [33, 1024], P(None, 'fsdp')
- ln1_gain: bfloat16 [1024], P('fsdp')
- ln1_bias: bfloat16 [1024], P('fsdp')
- w_qkv: bfloat16 [1024, 3072], P('fsdp')
- b_qkv: bfloat16 [3072], P('fsdp')
- w_out: bfloat16 [1024, 1024], P('fsdp')
- b_out: bfloat16 [1024], P('fsdp')
- ln2_gain: bfloat16 [1024], P('fsdp')
- ln2_bias: bfloat16 [1024], P('fsdp')
- w_fc1: bfloat16 [1024, 4096], P('fsdp')
- b_fc1: bfloat16 [4096], P('fsdp')
- w_fc2: bfloat16 [4096, 1024], P('fsdp')
- b_fc2: bfloat16 [1024], P('fsdp')
Outputs:
- output 1: bfloat16 [256, 256, 1024], P(('dp', 'fsdp'))
- output 2: float32 [33, 1024], P(None, 'fsdp')
- output 3: float32 [1024], P('fsdp')
- output 4: float32 [1024], P('fsdp')
- output 5: float32 [1024, 3072], P('fsdp')
- output 6: float32 [3072], P('fsdp')
- output 7: float32 [1024, 1024], P('fsdp')
- output 8: float32 [1024], P('fsdp')
- output 9: float32 [1024], P('fsdp')
- output 10: float32 [1024], P('fsdp')
- output 11: float32 [1024, 4096], P('fsdp')
- output 12: float32 [4096], P('fsdp')
- output 13: float32 [4096, 1024], P('fsdp')
- output 14: float32 [1024], P('fsdp')
All inputs are finite; a program needn't handle non-finite values.
Results may differ from the reference program's by a relative error of at most 0.0115973.
Values are sent between devices in bfloat16 or wider.
A program may use at most 1 GiB of HBM per device.

```python
import jax
import jax.numpy as jnp
from jax import lax

D = 1024
HEADS = 16
FF = 4096
SEQ = 256
BATCH = 256
VOCAB = 33
CLS_ID = 0
PAD_ID = 1
EOS_ID = 2
MASK_ID = 32

HEAD_DIM = D // HEADS
MASK_RATIO = 0.15 * 0.8
LN_EPS = 1e-5
ROPE_BASE = 10000.0


def draw_tokens(tok_key):
    len_key, res_key, rate_key, pick_key = jax.random.split(tok_key, 4)
    lengths = jax.random.randint(len_key, (BATCH,), SEQ // 2, SEQ + 1)
    lengths = lengths.at[0].set(SEQ).at[1].set(SEQ // 2)
    position = jnp.arange(SEQ)[None, :]
    residues = jax.random.randint(res_key, (BATCH, SEQ), 4, 29)
    mask_rate = jax.random.randint(rate_key, (BATCH, 1), 5, 26)
    pick_draw = jax.random.randint(pick_key, (BATCH, SEQ), 0, 100)
    body_tok = jnp.where(pick_draw < mask_rate, MASK_ID, residues)
    last_pos = lengths[:, None] - 1
    tok_grid = jnp.where(position < last_pos, body_tok, PAD_ID)
    tok_grid = jnp.where(position == last_pos, EOS_ID, tok_grid)
    return jnp.where(position == 0, CLS_ID, tok_grid).astype(jnp.int32)


def setup_inputs(seed: int = 0) -> dict:
    keys = jax.random.split(jax.random.key(seed), 16)

    def draw_normal(sub_key, dims, std_scale, offset=0.0):
        return (jax.random.normal(sub_key, dims, jnp.float32) * std_scale + offset).astype(jnp.bfloat16)

    return {
        'tokens': draw_tokens(keys[0]),
        'grad_y': draw_normal(keys[1], (BATCH, SEQ, D), 1.0),
        'embedding': draw_normal(keys[2], (VOCAB, D), 1.0),
        'ln1_gain': draw_normal(keys[3], (D,), 0.2, 1.0),
        'ln1_bias': draw_normal(keys[4], (D,), 0.2),
        'w_qkv': draw_normal(keys[5], (D, 3 * D), D ** -0.5),
        'b_qkv': draw_normal(keys[6], (3 * D,), 0.2),
        'w_out': draw_normal(keys[7], (D, D), D ** -0.5),
        'b_out': draw_normal(keys[8], (D,), 0.2),
        'ln2_gain': draw_normal(keys[9], (D,), 0.2, 1.0),
        'ln2_bias': draw_normal(keys[10], (D,), 0.2),
        'w_fc1': draw_normal(keys[11], (D, FF), D ** -0.5),
        'b_fc1': draw_normal(keys[12], (FF,), 0.2),
        'w_fc2': draw_normal(keys[13], (FF, D), FF ** -0.5),
        'b_fc2': draw_normal(keys[14], (D,), 0.2),
    }


def to_bf16(x_val):
    return x_val.astype(jnp.bfloat16).astype(jnp.float32)


def mat_mul(lhs, rhs):
    return jnp.dot(lhs, rhs, preferred_element_type=jnp.float32)


def layer_norm(x_val, gain, bias):
    centered = x_val - jnp.mean(x_val, axis=-1, keepdims=True)
    row_var = jnp.mean(centered * centered, axis=-1, keepdims=True)
    return centered * lax.rsqrt(row_var + LN_EPS) * gain + bias


def rope_tables():
    inv_freq = 1.0 / (ROPE_BASE ** (jnp.arange(0, HEAD_DIM, 2, dtype=jnp.float32) / HEAD_DIM))
    angles = jnp.arange(SEQ, dtype=jnp.float32)[:, None] * inv_freq[None, :]
    return jnp.cos(angles)[:, None, :], jnp.sin(angles)[:, None, :]


def rotate(x_val, cos_tab, sin_tab):
    half_dim = x_val.shape[-1] // 2
    low_half = x_val[..., :half_dim]
    high_half = x_val[..., half_dim:]
    return jnp.concatenate([low_half * cos_tab - high_half * sin_tab, high_half * cos_tab + low_half * sin_tab], axis=-1)


def seq_forward(weights, tok_row):
    (embedding, ln1_gain, ln1_bias, w_qkv, b_qkv, w_out, b_out,
     ln2_gain, ln2_bias, w_fc1, b_fc1, w_fc2, b_fc2) = weights
    is_mask = tok_row == MASK_ID
    is_pad = tok_row == PAD_ID
    mask_count = jnp.sum(is_mask.astype(jnp.float32))
    real_count = jnp.sum(jnp.logical_not(is_pad).astype(jnp.float32))
    factor = (1.0 - MASK_RATIO) / (1.0 - mask_count / real_count)
    keep_scale = jnp.where(is_mask | is_pad, 0.0, factor)
    x_in = to_bf16(embedding[tok_row] * keep_scale[:, None])
    h_one = to_bf16(layer_norm(x_in, ln1_gain, ln1_bias))
    qkv_proj = (mat_mul(h_one, w_qkv) + b_qkv).reshape(SEQ, 3, HEADS, HEAD_DIM)
    cos_tab, sin_tab = rope_tables()
    queries = to_bf16(rotate(qkv_proj[:, 0] * HEAD_DIM ** -0.5, cos_tab, sin_tab))
    key_rows = to_bf16(rotate(qkv_proj[:, 1], cos_tab, sin_tab))
    values = to_bf16(qkv_proj[:, 2])
    scores = jnp.einsum('qhd,khd->hqk', queries, key_rows)
    scores = jnp.where(is_pad[None, None, :], -1e30, scores)
    attn_prob = to_bf16(jax.nn.softmax(scores, axis=-1))
    context = to_bf16(jnp.einsum('hqk,khd->qhd', attn_prob, values)).reshape(SEQ, D)
    x_mid = x_in + mat_mul(context, w_out) + b_out
    h_two = to_bf16(layer_norm(x_mid, ln2_gain, ln2_bias))
    hidden_act = to_bf16(jax.nn.gelu(mat_mul(h_two, w_fc1) + b_fc1, approximate=False))
    return to_bf16(x_mid + mat_mul(hidden_act, w_fc2) + b_fc2)


def reference(tokens, grad_y, embedding, ln1_gain, ln1_bias, w_qkv, b_qkv, w_out, b_out,
              ln2_gain, ln2_bias, w_fc1, b_fc1, w_fc2, b_fc2):
    weights = tuple(w.astype(jnp.float32) for w in (embedding, ln1_gain, ln1_bias, w_qkv, b_qkv, w_out, b_out,
                                                     ln2_gain, ln2_bias, w_fc1, b_fc1, w_fc2, b_fc2))
    grad_init = tuple(jnp.zeros_like(w) for w in weights)

    def scan_step(grad_sum, seq_pair):
        tok_row, dy_row = seq_pair
        y_row, pull_back = jax.vjp(lambda params: seq_forward(params, tok_row), weights)
        grad_row = pull_back(dy_row.astype(jnp.float32))[0]
        new_sum = tuple(a_sum + g_row for a_sum, g_row in zip(grad_sum, grad_row))
        return new_sum, y_row.astype(jnp.bfloat16)

    grad_total, hidden = lax.scan(scan_step, grad_init, (tokens, grad_y))
    return (hidden,) + tuple(grad_total)
```

```python
import functools
import jax
import jax.numpy as jnp
from jax import lax
from jax.experimental import pallas as pl
from jax.experimental.pallas import tpu as pltpu
from jax.sharding import PartitionSpec as P

HEAD_DIM = 64
HALF = 32
MASK_ID = 32
PAD_ID = 1
TAB = 32
MASK_RATIO = 0.15 * 0.8
LN_EPS = 1e-5
ROPE_BASE = 10000.0
F32 = jnp.float32
BF16 = jnp.bfloat16
NEG = -1e30
MIB = 1024 * 1024


def dot(lhs, rhs, lhs_dim=1, rhs_dim=0):
    return lax.dot_general(lhs, rhs, (((lhs_dim,), (rhs_dim,)), ((), ())), preferred_element_type=F32)


def split_two(val):
    high = val.astype(BF16)
    return high, (val - high.astype(F32)).astype(BF16)


def one_hot_t(tok_row, rows):
    index = lax.broadcasted_iota(jnp.int32, (rows, tok_row.shape[1]), 0) & (TAB - 1)
    return jnp.where(index == tok_row, 1.0, 0.0).astype(BF16)


def attn_fwd_kernel(len_ref, tok_ref, tab_ref, cos_ref, sin_ref, qkv_ref, ctx_ref, lse_ref, s_a, s_b, p_a, p_b):
    model = ctx_ref.shape[1]
    seq = ctx_ref.shape[0]
    split = seq // 2
    pairs = model // 128
    length = len_ref[pl.program_id(0)]
    hot = one_hot_t(tok_ref[0], 3 * TAB)
    cos_tab, sin_tab = cos_ref[...], sin_ref[...]
    wide = 256

    def expand(step, carry):
        offset = pl.multiple_of(step * wide, wide)
        part = tab_ref[0, :, pl.ds(offset, wide)]
        high = part.astype(BF16)
        rest = part - high.astype(F32)
        mid = rest.astype(BF16)
        low = (rest - mid.astype(F32)).astype(BF16)
        raw = dot(jnp.concatenate([high, mid, low], axis=0), hot, 0, 0)
        for head in range(wide // HEAD_DIM):
            low_half = raw[head * HEAD_DIM:head * HEAD_DIM + HALF]
            high_half = raw[head * HEAD_DIM + HALF:(head + 1) * HEAD_DIM]
            turned = jnp.concatenate([low_half * cos_tab - high_half * sin_tab,
                                      high_half * cos_tab + low_half * sin_tab], axis=0).astype(BF16)
            qkv_ref[0, pl.ds(pl.multiple_of(offset + head * HEAD_DIM, HEAD_DIM), HEAD_DIM), :] = turned
        return carry

    def expand_v(step, carry):
        offset = pl.multiple_of(2 * model + step * wide, wide)
        part = tab_ref[0, :, pl.ds(offset, wide)].astype(BF16)
        qkv_ref[0, pl.ds(offset, wide), :] = dot(part, hot[:TAB], 0, 0).astype(BF16)
        return carry

    lax.fori_loop(0, 2 * model // wide, expand, 0, unroll=4)
    lax.fori_loop(0, model // wide, expand_v, 0, unroll=4)

    def head_rows(part, step, sub):
        return pl.ds(pl.multiple_of(part * model + step * 128 + sub * HEAD_DIM, HEAD_DIM), HEAD_DIM)

    def score(dst, step):
        for sub in range(2):
            dst[sub] = dot(qkv_ref[0, head_rows(1, step, sub), :], qkv_ref[0, head_rows(0, step, sub), :], 0, 0)

    def soften(src, dst, step):
        key_ok = lax.broadcasted_iota(jnp.int32, (seq - split, seq), 0) + split < length
        for sub in range(2):
            first = src[sub, :split]
            last = jnp.where(key_ok, src[sub, split:], NEG)
            top = jnp.maximum(jnp.max(first, axis=0, keepdims=True), jnp.max(last, axis=0, keepdims=True))
            first, last = jnp.exp(first - top), jnp.exp(last - top)
            total = jnp.sum(first, axis=0, keepdims=True) + jnp.sum(last, axis=0, keepdims=True)
            inverse = 1.0 / total
            dst[sub, :split] = (first * inverse).astype(BF16)
            dst[sub, split:] = (last * inverse).astype(BF16)
            lse_ref[0, pl.ds(2 * step + sub, 1), :] = top + jnp.log(total)

    def context(src, step):
        outs = [dot(qkv_ref[0, head_rows(2, step, sub), :], src[sub]) for sub in range(2)]
        ctx_ref[:, pl.ds(pl.multiple_of(step * 128, 128), 128)] = jnp.concatenate(outs, axis=0).T.astype(BF16)

    score(s_a, 0)

    def two_pairs(step, carry):
        even = 2 * step
        score(s_b, even + 1)
        context(p_b, (even + pairs - 1) & (pairs - 1))
        soften(s_a, p_a, even)
        score(s_a, (even + 2) & (pairs - 1))
        context(p_a, even)
        soften(s_b, p_b, even + 1)
        return carry

    lax.fori_loop(0, pairs // 2, two_pairs, 0)
    context(p_b, pairs - 1)


def attn_bwd_kernel(len_ref, tok_ref, qkv_ref, lse_ref, dctx_ref, cos_ref, sin_ref, high_ref, low_ref, bias_ref,
                    s_a, s_b, d_a, d_b, p_a, p_b, g_a, g_b, dct):
    model = dctx_ref.shape[1]
    seq = dctx_ref.shape[0]
    split = seq // 2
    pairs = model // 128
    length = len_ref[pl.program_id(0)]
    hot = one_hot_t(tok_ref[0], TAB)
    cos_tab, sin_tab = cos_ref[...], sin_ref[...]

    @pl.when(pl.program_id(0) == 0)
    def _():
        bias_ref[...] = jnp.zeros_like(bias_ref)
        p_b[...] = jnp.zeros_like(p_b)
        g_b[...] = jnp.zeros_like(g_b)

    def flip(step, carry):
        offset = pl.multiple_of(step * 128, 128)
        dct[pl.ds(offset, 128), :] = dctx_ref[:, pl.ds(offset, 128)].T
        return carry

    lax.fori_loop(0, pairs, flip, 0, unroll=4)

    def head_rows(part, step, sub):
        return pl.ds(pl.multiple_of(part * model + step * 128 + sub * HEAD_DIM, HEAD_DIM), HEAD_DIM)

    def unrope(val):
        low, high = val[:HALF], val[HALF:]
        return jnp.concatenate([low * cos_tab + high * sin_tab, high * cos_tab - low * sin_tab], axis=0)

    def put(offset, grad, fresh):
        offset = pl.multiple_of(offset, 128)
        folded = grad[:, :128]
        for lane in range(128, seq, 128):
            folded += grad[:, lane:lane + 128]
        bias_ref[pl.ds(offset, 128), :] += folded * fresh
        sums = dot(hot, grad.astype(BF16), 1, 1)
        high, low = split_two(sums)
        high_ref[0, :, pl.ds(offset, 128)] = high
        low_ref[0, :, pl.ds(offset, 128)] = low

    def score(dst_s, dst_d, step):
        for sub in range(2):
            dst_s[sub] = dot(qkv_ref[0, head_rows(1, step, sub), :], qkv_ref[0, head_rows(0, step, sub), :], 0, 0)
            dst_d[sub] = dot(qkv_ref[0, head_rows(2, step, sub), :], dct[head_rows(0, step, sub), :], 0, 0)

    def soften(src_s, src_d, dst_p, dst_g, step):
        key_ok = lax.broadcasted_iota(jnp.int32, (seq - split, seq), 0) + split < length
        for sub in range(2):
            lse = lse_ref[0, pl.ds(2 * step + sub, 1), :]
            first = jnp.exp(src_s[sub, :split] - lse)
            last = jnp.exp(jnp.where(key_ok, src_s[sub, split:], NEG) - lse)
            dst_p[sub, :split] = first.astype(BF16)
            dst_p[sub, split:] = last.astype(BF16)
            d_first, d_last = src_d[sub, :split], src_d[sub, split:]
            delta = jnp.sum(d_first * first, axis=0, keepdims=True) + jnp.sum(d_last * last, axis=0, keepdims=True)
            dst_g[sub, :split] = (first * (d_first - delta)).astype(BF16)
            dst_g[sub, split:] = (last * (d_last - delta)).astype(BF16)

    def grads(src_p, src_g, step, fresh):
        dq, dk, dv = [], [], []
        for sub in range(2):
            dv.append(dot(dct[head_rows(0, step, sub), :], src_p[sub], 1, 1))
            dq.append(unrope(dot(qkv_ref[0, head_rows(1, step, sub), :], src_g[sub])) * (HEAD_DIM ** -0.5))
            dk.append(unrope(dot(qkv_ref[0, head_rows(0, step, sub), :], src_g[sub], 1, 1)))
        put(step * 128, jnp.concatenate(dq, axis=0), fresh)
        put(model + step * 128, jnp.concatenate(dk, axis=0), fresh)
        put(2 * model + step * 128, jnp.concatenate(dv, axis=0), fresh)

    score(s_a, d_a, 0)

    def two_pairs(step, carry):
        even = 2 * step
        score(s_b, d_b, even + 1)
        grads(p_b, g_b, (even + pairs - 1) & (pairs - 1), jnp.where(step == 0, 0.0, 1.0))
        soften(s_a, d_a, p_a, g_a, even)
        score(s_a, d_a, (even + 2) & (pairs - 1))
        grads(p_a, g_a, even, 1.0)
        soften(s_b, d_b, p_b, g_b, even + 1)
        return carry

    lax.fori_loop(0, pairs // 2, two_pairs, 0)
    grads(p_b, g_b, pairs - 1, 1.0)


def fold_rows(val):
    return jnp.sum(val.reshape(val.shape[0] // 8, 8, val.shape[1]), axis=0)


def row_stats(val):
    centered = val - jnp.mean(val, axis=-1, keepdims=True)
    inv_std = lax.rsqrt(jnp.mean(centered * centered, axis=-1, keepdims=True) + LN_EPS)
    return centered * inv_std, inv_std


def mid_kernel(tok_ref, ctx_ref, w_ref, tab_ref, bias_ref, gain_ref, shift_ref, xmid_ref, h_ref):
    seq = tok_ref.shape[2]
    for part in range(tok_ref.shape[0]):
        rows = slice(part * seq, (part + 1) * seq)
        hot = one_hot_t(tok_ref[part], TAB)
        x_in = dot(hot, tab_ref[part], 0, 0)
        x_mid = x_in + dot(ctx_ref[rows, :], w_ref[...]) + bias_ref[...]
        xmid_ref[rows, :] = x_mid
        x_hat, _ = row_stats(x_mid)
        h_ref[rows, :] = (x_hat * gain_ref[...] + shift_ref[...]).astype(BF16)


def mlp_kernel(h_ref, dy_ref, w1_ref, w2_ref, b1_ref, act_ref, dpre_ref, gb_ref):
    width = act_ref.shape[1]
    tile = 256

    @pl.when(pl.program_id(1) == 0)
    def _():
        gb_ref[...] = jnp.zeros_like(gb_ref)

    for start in range(0, width, tile):
        cols = slice(start, start + tile)
        pre = dot(h_ref[...], w1_ref[:, cols]) + b1_ref[:, cols]
        d_act = dot(dy_ref[...], w2_ref[cols, :], 1, 1)
        phi = 0.5 + 0.5 * lax.erf(pre * (2.0 ** -0.5))
        act_ref[:, cols] = (pre * phi).astype(BF16)
        slope = phi + pre * (jnp.exp(pre * pre * -0.5) * 0.3989422804014327)
        d_pre = d_act * slope
        gb_ref[:, cols] += fold_rows(d_pre)
        dpre_ref[:, cols] = d_pre.astype(BF16)


def back_kernel(tok_ref, dpre_ref, w1_ref, xmid_ref, dy_ref, wout_ref, gain_ref,
                dmid_ref, dctx_ref, seg_ref, ggain_ref, gshift_ref, gbout_ref, gbfc2_ref):
    seq = tok_ref.shape[2]

    @pl.when(pl.program_id(0) == 0)
    def _():
        for ref in (ggain_ref, gshift_ref, gbout_ref, gbfc2_ref):
            ref[...] = jnp.zeros_like(ref)

    for part in range(tok_ref.shape[0]):
        rows = slice(part * seq, (part + 1) * seq)
        d_two = dot(dpre_ref[rows, :], w1_ref[...], 1, 1)
        x_hat, inv_std = row_stats(xmid_ref[rows, :])
        grad_y = dy_ref[rows, :].astype(F32)
        d_hat = d_two * gain_ref[...]
        d_x = inv_std * (d_hat - jnp.mean(d_hat, axis=-1, keepdims=True)
                         - x_hat * jnp.mean(d_hat * x_hat, axis=-1, keepdims=True))
        d_mid = grad_y + d_x
        ggain_ref[...] += fold_rows(d_two * x_hat)
        gshift_ref[...] += fold_rows(d_two)
        gbout_ref[...] += fold_rows(d_mid)
        gbfc2_ref[...] += fold_rows(grad_y)
        high, low = split_two(d_mid)
        dmid_ref[rows, :] = high
        hot = one_hot_t(tok_ref[part], TAB)
        seg_ref[part] = dot(hot, high) + dot(hot, low)
        dctx_ref[rows, :] = dot(high, wout_ref[...], 1, 1).astype(BF16)


def whole(shape):
    return pl.BlockSpec(shape, lambda *_: (0,) * len(shape), pipeline_mode=pl.Buffered(1))


def cost(flops, nbytes):
    return pl.CostEstimate(flops=int(flops), bytes_accessed=int(nbytes), transcendentals=0)


def params(dims, limit=56):
    return pltpu.CompilerParams(dimension_semantics=dims, vmem_limit_bytes=limit * MIB)


def run_attn_fwd(lengths, tok_rows, tab, cos_tab, sin_tab, seq, model):
    batch = tok_rows.shape[0]
    heads = model // HEAD_DIM
    return pl.pallas_call(
        attn_fwd_kernel, grid=(batch,), name='attn_fwd',
        in_specs=[pl.BlockSpec(memory_space=pltpu.SMEM),
                  pl.BlockSpec((1, 1, seq), lambda b: (b, 0, 0)),
                  pl.BlockSpec((1, TAB, 3 * model), lambda b: (b, 0, 0)),
                  whole((HALF, seq)), whole((HALF, seq))],
        out_specs=[pl.BlockSpec((1, 3 * model, seq), lambda b: (b, 0, 0)),
                   pl.BlockSpec((seq, model), lambda b: (b, 0)),
                   pl.BlockSpec((1, heads, seq), lambda b: (b, 0, 0))],
        out_shape=[jax.ShapeDtypeStruct((batch, 3 * model, seq), BF16),
                   jax.ShapeDtypeStruct((batch * seq, model), BF16),
                   jax.ShapeDtypeStruct((batch, heads, seq), F32)],
        scratch_shapes=[pltpu.VMEM((2, seq, seq), F32)] * 2 + [pltpu.VMEM((2, seq, seq), BF16)] * 2,
        cost_estimate=cost(60e9 * 0.75, 60e6),
        compiler_params=params(('arbitrary',)))(lengths, tok_rows, tab, cos_tab, sin_tab)


def run_attn_bwd(lengths, tok_rows, qkv_t, lse, d_ctx, cos_tab, sin_tab, seq, model):
    batch = tok_rows.shape[0]
    heads = model // HEAD_DIM
    return pl.pallas_call(
        attn_bwd_kernel, grid=(batch,), name='attn_bwd',
        in_specs=[pl.BlockSpec(memory_space=pltpu.SMEM),
                  pl.BlockSpec((1, 1, seq), lambda b: (b, 0, 0)),
                  pl.BlockSpec((1, 3 * model, seq), lambda b: (b, 0, 0)),
                  pl.BlockSpec((1, heads, seq), lambda b: (b, 0, 0)),
                  pl.BlockSpec((seq, model), lambda b: (b, 0)),
                  whole((HALF, seq)), whole((HALF, seq))],
        out_specs=[pl.BlockSpec((1, TAB, 3 * model), lambda b: (b, 0, 0)),
                   pl.BlockSpec((1, TAB, 3 * model), lambda b: (b, 0, 0)),
                   pl.BlockSpec((3 * model, 128), lambda b: (0, 0))],
        out_shape=[jax.ShapeDtypeStruct((batch, TAB, 3 * model), BF16),
                   jax.ShapeDtypeStruct((batch, TAB, 3 * model), BF16),
                   jax.ShapeDtypeStruct((3 * model, 128), F32)],
        scratch_shapes=[pltpu.VMEM((2, seq, seq), F32)] * 4 + [pltpu.VMEM((2, seq, seq), BF16)] * 4
        + [pltpu.VMEM((model, seq), BF16)],
        cost_estimate=cost(110e9 * 0.75, 60e6),
        compiler_params=params(('arbitrary',)))(lengths, tok_rows, qkv_t, lse, d_ctx, cos_tab, sin_tab)


def run_mid(tok_rows, ctx, w_out, x_tab, b_out, gain, shift, seq, model):
    batch = tok_rows.shape[0]
    rows = batch * seq
    group = 2
    tile = group * seq
    return pl.pallas_call(
        mid_kernel, grid=(batch // group,), name='mid',
        in_specs=[pl.BlockSpec((group, 1, seq), lambda b: (b, 0, 0)),
                  pl.BlockSpec((tile, model), lambda b: (b, 0)),
                  whole((model, model)),
                  pl.BlockSpec((group, TAB, model), lambda b: (b, 0, 0)),
                  whole((1, model)), whole((1, model)), whole((1, model))],
        out_specs=[pl.BlockSpec((tile, model), lambda b: (b, 0)),
                   pl.BlockSpec((tile, model), lambda b: (b, 0))],
        out_shape=[jax.ShapeDtypeStruct((rows, model), F32), jax.ShapeDtypeStruct((rows, model), BF16)],
        cost_estimate=cost(2 * rows * model * model, rows * model * 8),
        compiler_params=params(('arbitrary',)))(tok_rows, ctx, w_out, x_tab, b_out, gain, shift)


def run_mlp(h_two, grad_y, w_fc1, w_fc2, b_fc1):
    rows, model = h_two.shape
    width = w_fc1.shape[1]
    tile, cols = 512, 1024
    return pl.pallas_call(
        mlp_kernel, grid=(width // cols, rows // tile), name='mlp',
        in_specs=[pl.BlockSpec((tile, model), lambda f, r: (r, 0)),
                  pl.BlockSpec((tile, model), lambda f, r: (r, 0)),
                  pl.BlockSpec((model, cols), lambda f, r: (0, f)),
                  pl.BlockSpec((cols, model), lambda f, r: (f, 0)),
                  pl.BlockSpec((1, cols), lambda f, r: (0, f))],
        out_specs=[pl.BlockSpec((tile, cols), lambda f, r: (r, f)),
                   pl.BlockSpec((tile, cols), lambda f, r: (r, f)),
                   pl.BlockSpec((8, cols), lambda f, r: (0, f))],
        out_shape=[jax.ShapeDtypeStruct((rows, width), BF16), jax.ShapeDtypeStruct((rows, width), BF16),
                   jax.ShapeDtypeStruct((8, width), F32)],
        cost_estimate=cost(4 * rows * model * width, 134e6),
        compiler_params=params(('arbitrary', 'arbitrary')))(h_two, grad_y, w_fc1, w_fc2, b_fc1)


def run_back(tok_rows, d_pre, w_fc1, x_mid, grad_y, w_out, gain, seq, model):
    batch = tok_rows.shape[0]
    rows, width = d_pre.shape
    group = 2
    tile = group * seq
    vec = jax.ShapeDtypeStruct((8, model), F32)
    vec_spec = pl.BlockSpec((8, model), lambda b: (0, 0))
    row_spec = pl.BlockSpec((tile, model), lambda b: (b, 0))
    return pl.pallas_call(
        back_kernel, grid=(batch // group,), name='back',
        in_specs=[pl.BlockSpec((group, 1, seq), lambda b: (b, 0, 0)),
                  pl.BlockSpec((tile, width), lambda b: (b, 0)),
                  whole((model, width)), row_spec, row_spec, whole((model, model)), whole((1, model))],
        out_specs=[row_spec, row_spec, pl.BlockSpec((group, TAB, model), lambda b: (b, 0, 0)),
                   vec_spec, vec_spec, vec_spec, vec_spec],
        out_shape=[jax.ShapeDtypeStruct((rows, model), BF16), jax.ShapeDtypeStruct((rows, model), BF16),
                   jax.ShapeDtypeStruct((batch, TAB, model), F32), vec, vec, vec, vec],
        cost_estimate=cost(2 * rows * model * (width + model), 90e6),
        compiler_params=params(('arbitrary',)))(tok_rows, d_pre, w_fc1, x_mid, grad_y, w_out, gain)


def solution(mesh):
    row_spec = P(('dp', 'fsdp'), None)
    act_spec = P(('dp', 'fsdp'), None, None)
    param_specs = (P(None, 'fsdp'),) + (P('fsdp'),) * 12
    swap = [(0, 1), (1, 0)]

    def local_step(tokens, grad_y3, *shards):
        (e_part, gain1_part, shift1_part, wqkv_part, bqkv_part, wout_part, bout_part,
         gain2_part, shift2_part, wfc1_part, bfc1_part, wfc2_part, bfc2_part) = shards
        batch, seq = tokens.shape
        vocab = e_part.shape[0]
        model = grad_y3.shape[2]

        def gather(part):
            return lax.all_gather(part, 'fsdp', axis=0, tiled=True)

        smalls = (gain1_part, shift1_part, bout_part, gain2_part, shift2_part, bfc2_part, bqkv_part, bfc1_part)
        packed = jnp.concatenate([e_part] + [part.reshape(-1, 128) for part in smalls], axis=0)
        packed = lax.all_gather(packed, 'fsdp', axis=0, tiled=False)
        w_qkv, w_out, w_fc1, w_fc2 = (gather(part) for part in (wqkv_part, wout_part, wfc1_part, wfc2_part))
        table = packed[:, :vocab].transpose(1, 0, 2).reshape(vocab, model)[:TAB]
        vecs, at = [], vocab
        for part in smalls:
            count = part.shape[0] // 128
            vecs.append(packed[:, at:at + count].reshape(1, -1).astype(F32))
            at += count
        gain1, shift1, b_out, gain2, shift2, b_fc2, b_qkv, b_fc1 = vecs
        grad_y = grad_y3.reshape(batch * seq, model)

        is_mask, is_pad = tokens == MASK_ID, tokens == PAD_ID
        lengths = jnp.sum(jnp.logical_not(is_pad), axis=1).astype(jnp.int32)
        factor = (1.0 - MASK_RATIO) / (1.0 - jnp.sum(is_mask, axis=1).astype(F32) / lengths.astype(F32))
        tok_rows = jnp.where(is_mask, PAD_ID, tokens)[:, None, :]
        keep = jnp.where(jnp.arange(TAB) == PAD_ID, 0.0, factor[:, None])[:, :, None]
        x_tab = (table.astype(F32)[None] * keep).astype(BF16)
        hat_one, inv_one = row_stats(x_tab.astype(F32))
        h_tab = (hat_one * gain1 + shift1).astype(BF16).reshape(batch * TAB, model)
        scale = jnp.where(jnp.arange(3 * model) < model, HEAD_DIM ** -0.5, 1.0)[None]
        qkv_tab = ((dot(h_tab, w_qkv) + b_qkv) * scale).reshape(batch, TAB, 3 * model)

        inv_freq = 1.0 / (ROPE_BASE ** (jnp.arange(0, HEAD_DIM, 2, dtype=F32) / HEAD_DIM))
        angles = inv_freq[:, None] * jnp.arange(seq, dtype=F32)[None, :]
        cos_tab, sin_tab = jnp.cos(angles), jnp.sin(angles)

        qkv_t, ctx, lse = run_attn_fwd(lengths, tok_rows, qkv_tab, cos_tab, sin_tab, seq, model)
        x_mid, h_two = run_mid(tok_rows, ctx, w_out, x_tab, b_out, gain2, shift2, seq, model)
        act, d_pre, gb_fc1 = run_mlp(h_two, grad_y, w_fc1, w_fc2, b_fc1)

        me = lax.axis_index('fsdp')
        spot = {1: me & 1, 2: (me >> 1) & 1, 4: me >> 2}

        def over_dp(part):
            return part + lax.ppermute(part, 'dp', swap)

        def scatter(grad):
            return lax.psum_scatter(grad, 'fsdp', scatter_dimension=0, tiled=True)

        def parts_of(val, bit, axis):
            send = lax.dynamic_index_in_dim(val, 1 - spot[bit], axis, keepdims=False)
            return send, lax.dynamic_index_in_dim(val, spot[bit], axis, keepdims=False)

        def trade(send, bit):
            return lax.ppermute(send, 'fsdp', [(dev, dev ^ bit) for dev in range(8)])

        after = lax.optimization_barrier
        raw_fc2 = dot(act, grad_y, 0, 0)
        part_fc2 = scatter(raw_fc2)
        h_two, d_pre, raw_fc2 = after((h_two, d_pre, raw_fc2))
        raw_fc1 = dot(h_two, d_pre, 0, 0)
        rows = raw_fc1.shape[0] // 8
        send, held = parts_of(raw_fc1.reshape(2, 2, 2, rows, raw_fc1.shape[1]), 1, 2)
        d_pre, send = after((d_pre, send))
        got = trade(send, 1)
        d_mid, d_ctx, seg_mid, gg2, gs2, gb_out, gb_fc2 = run_back(
            tok_rows, d_pre, w_fc1, x_mid, grad_y, w_out, gain2, seq, model)
        d_mid, got = after((d_mid, got))
        total = held + got
        send_a, held_a = parts_of(total[:, :, :rows // 2], 2, 1)
        send_b, held_b = parts_of(total[:, :, rows // 2:], 4, 0)
        d_mid, send_a, send_b = after((d_mid, send_a, send_b))
        got_a, got_b = trade(send_a, 2), trade(send_b, 4)
        raw_out = dot(ctx, d_mid, 0, 0)
        part_out = scatter(raw_out)
        d_ctx, raw_out, part_fc2 = after((d_ctx, raw_out, part_fc2))
        g_w_fc2 = over_dp(part_fc2)
        d_high, d_low, gb_qkv = run_attn_bwd(lengths, tok_rows, qkv_t, lse, d_ctx, cos_tab, sin_tab, seq, model)
        d_high, got_a, got_b, part_out, g_w_fc2 = after((d_high, got_a, got_b, part_out, g_w_fc2))
        g_w_out = over_dp(part_out)
        send_a, held_a = parts_of(held_a + got_a, 4, 0)
        send_b, held_b = parts_of(held_b + got_b, 2, 0)
        d_high, send_a, send_b = after((d_high, send_a, send_b))
        got_a, got_b = trade(send_a, 4), trade(send_b, 2)
        d_tab = jnp.concatenate([d_high, d_low], axis=0).reshape(2 * batch * TAB, 3 * model)
        raw_qkv = dot(jnp.concatenate([h_tab, h_tab], axis=0), d_tab, 0, 0)
        part_qkv = scatter(raw_qkv)
        d_tab, raw_qkv, got_a, got_b = after((d_tab, raw_qkv, got_a, got_b))
        part_fc1 = jnp.concatenate([held_a + got_a, held_b + got_b], axis=0)
        d_tab, part_fc1, act = after((d_tab, part_fc1, act))
        g_w_fc1 = over_dp(part_fc1)
        d_one = dot(d_tab, w_qkv, 1, 1).reshape(2, batch, TAB, model)
        d_one = d_one[0] + d_one[1]
        d_hat = d_one * gain1
        d_x = inv_one * (d_hat - jnp.mean(d_hat, axis=-1, keepdims=True)
                         - hat_one * jnp.mean(d_hat * hat_one, axis=-1, keepdims=True))
        g_table = jnp.sum((seg_mid + d_x) * keep, axis=0)
        g_table = jnp.concatenate([g_table, jnp.zeros((vocab - TAB, model), F32)], axis=0)
        vec_grads = (jnp.sum(d_one * hat_one, axis=(0, 1)), jnp.sum(d_one, axis=(0, 1)), jnp.sum(gb_out, axis=0),
                     jnp.sum(gg2, axis=0), jnp.sum(gs2, axis=0), jnp.sum(gb_fc2, axis=0),
                     jnp.sum(gb_qkv, axis=1), jnp.sum(gb_fc1, axis=0))
        small = jnp.concatenate(
            [g_table.reshape(vocab, 8, 128).transpose(1, 0, 2)]
            + [vec.reshape(8, -1, 128) for vec in vec_grads], axis=1)
        small = lax.psum(small, ('dp', 'fsdp'))
        small = lax.dynamic_index_in_dim(small, me, 0, keepdims=False)
        g_small, at = [], vocab
        for part in smalls:
            count = part.shape[0] // 128
            g_small.append(small[at:at + count].reshape(-1))
            at += count
        gg1, gs1, gbo, ggn2, gsh2, gb2, gbq, gb1 = g_small
        hidden = (x_mid + dot(act, w_fc2) + b_fc2).astype(BF16)
        hidden, part_qkv = after((hidden, part_qkv))
        g_w_qkv = over_dp(part_qkv)
        hidden = hidden.reshape(grad_y3.shape)
        return (hidden, small[:vocab], gg1, gs1, g_w_qkv, gbq, g_w_out, gbo, ggn2, gsh2, g_w_fc1, gb1, g_w_fc2, gb2)

    return jax.shard_map(local_step, mesh=mesh, in_specs=(row_spec, act_spec) + param_specs,
                         out_specs=(act_spec,) + param_specs, check_vma=False)
```

```python
import functools
import jax
import jax.numpy as jnp
from jax import lax
from jax.experimental import pallas as pl
from jax.experimental.pallas import tpu as pltpu
from jax.sharding import PartitionSpec as P

HEAD_DIM = 64
HALF = 32
MASK_ID = 32
PAD_ID = 1
TAB = 32
MASK_RATIO = 0.15 * 0.8
LN_EPS = 1e-5
ROPE_BASE = 10000.0
F32 = jnp.float32
BF16 = jnp.bfloat16
NEG = -1e30
MIB = 1024 * 1024


def dot(lhs, rhs, lhs_dim=1, rhs_dim=0):
    return lax.dot_general(lhs, rhs, (((lhs_dim,), (rhs_dim,)), ((), ())), preferred_element_type=F32)


def split_two(val):
    high = val.astype(BF16)
    return high, (val - high.astype(F32)).astype(BF16)


def one_hot_t(tok_row, rows):
    index = lax.broadcasted_iota(jnp.int32, (rows, tok_row.shape[1]), 0) & (TAB - 1)
    return jnp.where(index == tok_row, 1.0, 0.0).astype(BF16)


def attn_fwd_kernel(len_ref, tok_ref, tab_ref, cos_ref, sin_ref, qkv_ref, ctx_ref, lse_ref, s_a, s_b, p_a, p_b):
    model = ctx_ref.shape[1]
    seq = ctx_ref.shape[0]
    split = seq // 2
    pairs = model // 128
    length = len_ref[pl.program_id(0)]
    hot = one_hot_t(tok_ref[0], 3 * TAB)
    cos_tab, sin_tab = cos_ref[...], sin_ref[...]
    wide = 256

    def expand(step, carry):
        offset = pl.multiple_of(step * wide, wide)
        part = tab_ref[0, :, pl.ds(offset, wide)]
        high = part.astype(BF16)
        rest = part - high.astype(F32)
        mid = rest.astype(BF16)
        low = (rest - mid.astype(F32)).astype(BF16)
        raw = dot(jnp.concatenate([high, mid, low], axis=0), hot, 0, 0)
        for head in range(wide // HEAD_DIM):
            low_half = raw[head * HEAD_DIM:head * HEAD_DIM + HALF]
            high_half = raw[head * HEAD_DIM + HALF:(head + 1) * HEAD_DIM]
            turned = jnp.concatenate([low_half * cos_tab - high_half * sin_tab,
                                      high_half * cos_tab + low_half * sin_tab], axis=0).astype(BF16)
            qkv_ref[0, pl.ds(pl.multiple_of(offset + head * HEAD_DIM, HEAD_DIM), HEAD_DIM), :] = turned
        return carry

    def expand_v(step, carry):
        offset = pl.multiple_of(2 * model + step * wide, wide)
        part = tab_ref[0, :, pl.ds(offset, wide)].astype(BF16)
        qkv_ref[0, pl.ds(offset, wide), :] = dot(part, hot[:TAB], 0, 0).astype(BF16)
        return carry

    lax.fori_loop(0, 2 * model // wide, expand, 0, unroll=4)
    lax.fori_loop(0, model // wide, expand_v, 0, unroll=4)

    def head_rows(part, step, sub):
        return pl.ds(pl.multiple_of(part * model + step * 128 + sub * HEAD_DIM, HEAD_DIM), HEAD_DIM)

    def score(dst, step):
        for sub in range(2):
            dst[sub] = dot(qkv_ref[0, head_rows(1, step, sub), :], qkv_ref[0, head_rows(0, step, sub), :], 0, 0)

    def soften(src, dst, step):
        key_ok = lax.broadcasted_iota(jnp.int32, (seq - split, seq), 0) + split < length
        for sub in range(2):
            first = src[sub, :split]
            last = jnp.where(key_ok, src[sub, split:], NEG)
            top = jnp.maximum(jnp.max(first, axis=0, keepdims=True), jnp.max(last, axis=0, keepdims=True))
            first, last = jnp.exp(first - top), jnp.exp(last - top)
            total = jnp.sum(first, axis=0, keepdims=True) + jnp.sum(last, axis=0, keepdims=True)
            inverse = 1.0 / total
            dst[sub, :split] = (first * inverse).astype(BF16)
            dst[sub, split:] = (last * inverse).astype(BF16)
            lse_ref[0, pl.ds(2 * step + sub, 1), :] = top + jnp.log(total)

    def context(src, step):
        outs = [dot(qkv_ref[0, head_rows(2, step, sub), :], src[sub]) for sub in range(2)]
        ctx_ref[:, pl.ds(pl.multiple_of(step * 128, 128), 128)] = jnp.concatenate(outs, axis=0).T.astype(BF16)

    score(s_a, 0)

    def two_pairs(step, carry):
        even = 2 * step
        score(s_b, even + 1)
        context(p_b, (even + pairs - 1) & (pairs - 1))
        soften(s_a, p_a, even)
        score(s_a, (even + 2) & (pairs - 1))
        context(p_a, even)
        soften(s_b, p_b, even + 1)
        return carry

    lax.fori_loop(0, pairs // 2, two_pairs, 0)
    context(p_b, pairs - 1)


def attn_bwd_kernel(len_ref, tok_ref, qkv_ref, lse_ref, dctx_ref, cos_ref, sin_ref, high_ref, low_ref, bias_ref,
                    s_a, s_b, d_a, d_b, p_a, p_b, g_a, g_b, dct):
    model = dctx_ref.shape[1]
    seq = dctx_ref.shape[0]
    split = seq // 2
    pairs = model // 128
    length = len_ref[pl.program_id(0)]
    hot = one_hot_t(tok_ref[0], TAB)
    cos_tab, sin_tab = cos_ref[...], sin_ref[...]

    @pl.when(pl.program_id(0) == 0)
    def _():
        bias_ref[...] = jnp.zeros_like(bias_ref)
        p_b[...] = jnp.zeros_like(p_b)
        g_b[...] = jnp.zeros_like(g_b)

    def flip(step, carry):
        offset = pl.multiple_of(step * 128, 128)
        dct[pl.ds(offset, 128), :] = dctx_ref[:, pl.ds(offset, 128)].T
        return carry

    lax.fori_loop(0, pairs, flip, 0, unroll=4)

    def head_rows(part, step, sub):
        return pl.ds(pl.multiple_of(part * model + step * 128 + sub * HEAD_DIM, HEAD_DIM), HEAD_DIM)

    def unrope(val):
        low, high = val[:HALF], val[HALF:]
        return jnp.concatenate([low * cos_tab + high * sin_tab, high * cos_tab - low * sin_tab], axis=0)

    def put(offset, grad, fresh):
        offset = pl.multiple_of(offset, 128)
        folded = grad[:, :128]
        for lane in range(128, seq, 128):
            folded += grad[:, lane:lane + 128]
        bias_ref[pl.ds(offset, 128), :] += folded * fresh
        sums = dot(hot, grad.astype(BF16), 1, 1)
        high, low = split_two(sums)
        high_ref[0, :, pl.ds(offset, 128)] = high
        low_ref[0, :, pl.ds(offset, 128)] = low

    def score(dst_s, dst_d, step):
        for sub in range(2):
            dst_s[sub] = dot(qkv_ref[0, head_rows(1, step, sub), :], qkv_ref[0, head_rows(0, step, sub), :], 0, 0)
            dst_d[sub] = dot(qkv_ref[0, head_rows(2, step, sub), :], dct[head_rows(0, step, sub), :], 0, 0)

    def soften(src_s, src_d, dst_p, dst_g, step):
        key_ok = lax.broadcasted_iota(jnp.int32, (seq - split, seq), 0) + split < length
        for sub in range(2):
            lse = lse_ref[0, pl.ds(2 * step + sub, 1), :]
            first = jnp.exp(src_s[sub, :split] - lse)
            last = jnp.exp(jnp.where(key_ok, src_s[sub, split:], NEG) - lse)
            dst_p[sub, :split] = first.astype(BF16)
            dst_p[sub, split:] = last.astype(BF16)
            d_first, d_last = src_d[sub, :split], src_d[sub, split:]
            delta = jnp.sum(d_first * first, axis=0, keepdims=True) + jnp.sum(d_last * last, axis=0, keepdims=True)
            dst_g[sub, :split] = (first * (d_first - delta)).astype(BF16)
            dst_g[sub, split:] = (last * (d_last - delta)).astype(BF16)

    def grads(src_p, src_g, step, fresh):
        dq, dk, dv = [], [], []
        for sub in range(2):
            dv.append(dot(dct[head_rows(0, step, sub), :], src_p[sub], 1, 1))
            dq.append(unrope(dot(qkv_ref[0, head_rows(1, step, sub), :], src_g[sub])) * (HEAD_DIM ** -0.5))
            dk.append(unrope(dot(qkv_ref[0, head_rows(0, step, sub), :], src_g[sub], 1, 1)))
        put(step * 128, jnp.concatenate(dq, axis=0), fresh)
        put(model + step * 128, jnp.concatenate(dk, axis=0), fresh)
        put(2 * model + step * 128, jnp.concatenate(dv, axis=0), fresh)

    score(s_a, d_a, 0)

    def two_pairs(step, carry):
        even = 2 * step
        score(s_b, d_b, even + 1)
        grads(p_b, g_b, (even + pairs - 1) & (pairs - 1), jnp.where(step == 0, 0.0, 1.0))
        soften(s_a, d_a, p_a, g_a, even)
        score(s_a, d_a, (even + 2) & (pairs - 1))
        grads(p_a, g_a, even, 1.0)
        soften(s_b, d_b, p_b, g_b, even + 1)
        return carry

    lax.fori_loop(0, pairs // 2, two_pairs, 0)
    grads(p_b, g_b, pairs - 1, 1.0)


def fold_rows(val):
    return jnp.sum(val.reshape(val.shape[0] // 8, 8, val.shape[1]), axis=0)


def row_stats(val):
    centered = val - jnp.mean(val, axis=-1, keepdims=True)
    inv_std = lax.rsqrt(jnp.mean(centered * centered, axis=-1, keepdims=True) + LN_EPS)
    return centered * inv_std, inv_std


def flat(ref):
    return ref[...].reshape(-1, ref.shape[-1])


def mid_kernel(tok_ref, ctx_ref, w_ref, tab_ref, bias_ref, gain_ref, shift_ref, xmid_ref, h_ref):
    seq = tok_ref.shape[2]
    for part in range(tok_ref.shape[0]):
        rows = slice(part * seq, (part + 1) * seq)
        hot = one_hot_t(tok_ref[part], TAB)
        x_in = dot(hot, tab_ref[part], 0, 0)
        x_mid = x_in + dot(ctx_ref[rows, :], flat(w_ref)) + bias_ref[...]
        xmid_ref[rows, :] = x_mid
        x_hat, _ = row_stats(x_mid)
        h_ref[rows, :] = (x_hat * gain_ref[...] + shift_ref[...]).astype(BF16)


def mlp_kernel(h_ref, dy_ref, w1_ref, w2_ref, b1_ref, act_ref, dpre_ref, gb_ref):
    width = act_ref.shape[1]
    tile = 256

    @pl.when(pl.program_id(1) == 0)
    def _():
        gb_ref[...] = jnp.zeros_like(gb_ref)

    for start in range(0, width, tile):
        cols = slice(start, start + tile)
        pre = dot(h_ref[...], w1_ref[:, cols]) + b1_ref[:, cols]
        d_act = dot(dy_ref[...], w2_ref[start // tile], 1, 1)
        phi = 0.5 + 0.5 * lax.erf(pre * (2.0 ** -0.5))
        act_ref[:, cols] = (pre * phi).astype(BF16)
        slope = phi + pre * (jnp.exp(pre * pre * -0.5) * 0.3989422804014327)
        d_pre = d_act * slope
        gb_ref[:, cols] += fold_rows(d_pre)
        dpre_ref[:, cols] = d_pre.astype(BF16)


def back_kernel(tok_ref, dpre_a, dpre_b, w1_a, w1_b, xmid_ref, dy_ref, wout_ref, gain_ref,
                dmid_ref, dctx_ref, seg_ref, ggain_ref, gshift_ref, gbout_ref, gbfc2_ref):
    seq = tok_ref.shape[2]

    @pl.when(pl.program_id(0) == 0)
    def _():
        for ref in (ggain_ref, gshift_ref, gbout_ref, gbfc2_ref):
            ref[...] = jnp.zeros_like(ref)

    for part in range(tok_ref.shape[0]):
        rows = slice(part * seq, (part + 1) * seq)
        d_two = dot(dpre_a[rows, :], w1_a[...], 1, 1) + dot(dpre_b[rows, :], w1_b[...], 1, 1)
        x_hat, inv_std = row_stats(xmid_ref[rows, :])
        grad_y = dy_ref[rows, :].astype(F32)
        d_hat = d_two * gain_ref[...]
        d_x = inv_std * (d_hat - jnp.mean(d_hat, axis=-1, keepdims=True)
                         - x_hat * jnp.mean(d_hat * x_hat, axis=-1, keepdims=True))
        d_mid = grad_y + d_x
        ggain_ref[...] += fold_rows(d_two * x_hat)
        gshift_ref[...] += fold_rows(d_two)
        gbout_ref[...] += fold_rows(d_mid)
        gbfc2_ref[...] += fold_rows(grad_y)
        high, low = split_two(d_mid)
        dmid_ref[rows, :] = high
        hot = one_hot_t(tok_ref[part], TAB)
        seg_ref[part] = dot(hot, high) + dot(hot, low)
        dctx_ref[rows, :] = dot(high, flat(wout_ref), 1, 1).astype(BF16)


def whole(shape):
    return pl.BlockSpec(shape, lambda *_: (0,) * len(shape), pipeline_mode=pl.Buffered(1))


def out_block(model):
    return pl.BlockSpec((8, 128, model), lambda *_: (0, 2, 0), pipeline_mode=pl.Buffered(1))


def cost(flops, nbytes):
    return pl.CostEstimate(flops=int(flops), bytes_accessed=int(nbytes), transcendentals=0)


def params(dims, limit=56):
    return pltpu.CompilerParams(dimension_semantics=dims, vmem_limit_bytes=limit * MIB)


def run_attn_fwd(lengths, tok_rows, tab, cos_tab, sin_tab, seq, model):
    batch = tok_rows.shape[0]
    heads = model // HEAD_DIM
    return pl.pallas_call(
        attn_fwd_kernel, grid=(batch,), name='attn_fwd',
        in_specs=[pl.BlockSpec(memory_space=pltpu.SMEM),
                  pl.BlockSpec((1, 1, seq), lambda b: (b, 0, 0)),
                  pl.BlockSpec((1, TAB, 3 * model), lambda b: (b, 0, 0)),
                  whole((HALF, seq)), whole((HALF, seq))],
        out_specs=[pl.BlockSpec((1, 3 * model, seq), lambda b: (b, 0, 0)),
                   pl.BlockSpec((seq, model), lambda b: (b, 0)),
                   pl.BlockSpec((1, heads, seq), lambda b: (b, 0, 0))],
        out_shape=[jax.ShapeDtypeStruct((batch, 3 * model, seq), BF16),
                   jax.ShapeDtypeStruct((batch * seq, model), BF16),
                   jax.ShapeDtypeStruct((batch, heads, seq), F32)],
        scratch_shapes=[pltpu.VMEM((2, seq, seq), F32)] * 2 + [pltpu.VMEM((2, seq, seq), BF16)] * 2,
        cost_estimate=cost(60e9 * 0.75, 60e6),
        compiler_params=params(('arbitrary',)))(lengths, tok_rows, tab, cos_tab, sin_tab)


def run_attn_bwd(lengths, tok_rows, qkv_t, lse, d_ctx, cos_tab, sin_tab, seq, model):
    batch = tok_rows.shape[0]
    heads = model // HEAD_DIM
    return pl.pallas_call(
        attn_bwd_kernel, grid=(batch,), name='attn_bwd',
        in_specs=[pl.BlockSpec(memory_space=pltpu.SMEM),
                  pl.BlockSpec((1, 1, seq), lambda b: (b, 0, 0)),
                  pl.BlockSpec((1, 3 * model, seq), lambda b: (b, 0, 0)),
                  pl.BlockSpec((1, heads, seq), lambda b: (b, 0, 0)),
                  pl.BlockSpec((seq, model), lambda b: (b, 0)),
                  whole((HALF, seq)), whole((HALF, seq))],
        out_specs=[pl.BlockSpec((1, TAB, 3 * model), lambda b: (b, 0, 0)),
                   pl.BlockSpec((1, TAB, 3 * model), lambda b: (b, 0, 0)),
                   pl.BlockSpec((3 * model, 128), lambda b: (0, 0))],
        out_shape=[jax.ShapeDtypeStruct((batch, TAB, 3 * model), BF16),
                   jax.ShapeDtypeStruct((batch, TAB, 3 * model), BF16),
                   jax.ShapeDtypeStruct((3 * model, 128), F32)],
        scratch_shapes=[pltpu.VMEM((2, seq, seq), F32)] * 4 + [pltpu.VMEM((2, seq, seq), BF16)] * 4
        + [pltpu.VMEM((model, seq), BF16)],
        cost_estimate=cost(110e9 * 0.75, 60e6),
        compiler_params=params(('arbitrary',)))(lengths, tok_rows, qkv_t, lse, d_ctx, cos_tab, sin_tab)


def run_mid(tok_rows, ctx, w_out, x_tab, b_out, gain, shift, seq, model):
    batch = tok_rows.shape[0]
    rows = batch * seq
    group = 2
    tile = group * seq
    return pl.pallas_call(
        mid_kernel, grid=(batch // group,), name='mid',
        in_specs=[pl.BlockSpec((group, 1, seq), lambda b: (b, 0, 0)),
                  pl.BlockSpec((tile, model), lambda b: (b, 0)),
                  out_block(model),
                  pl.BlockSpec((group, TAB, model), lambda b: (b, 0, 0)),
                  whole((1, model)), whole((1, model)), whole((1, model))],
        out_specs=[pl.BlockSpec((tile, model), lambda b: (b, 0)),
                   pl.BlockSpec((tile, model), lambda b: (b, 0))],
        out_shape=[jax.ShapeDtypeStruct((rows, model), F32), jax.ShapeDtypeStruct((rows, model), BF16)],
        cost_estimate=cost(2 * rows * model * model, rows * model * 8),
        compiler_params=params(('arbitrary',)))(tok_rows, ctx, w_out, x_tab, b_out, gain, shift)


def run_mlp(h_two, grad_y, w_fc1, w_fc2, b_fc1, name):
    rows, model = h_two.shape
    width = w_fc1.shape[1]
    tile, cols = 512, 1024
    return pl.pallas_call(
        mlp_kernel, grid=(width // cols, rows // tile), name=name,
        in_specs=[pl.BlockSpec((tile, model), lambda f, r: (r, 0)),
                  pl.BlockSpec((tile, model), lambda f, r: (r, 0)),
                  pl.BlockSpec((model, cols), lambda f, r: (0, f)),
                  pl.BlockSpec((cols // 256, 256, model), lambda f, r: (f, 0, 0)),
                  pl.BlockSpec((1, cols), lambda f, r: (0, f))],
        out_specs=[pl.BlockSpec((tile, cols), lambda f, r: (r, f)),
                   pl.BlockSpec((tile, cols), lambda f, r: (r, f)),
                   pl.BlockSpec((8, cols), lambda f, r: (0, f))],
        out_shape=[jax.ShapeDtypeStruct((rows, width), BF16), jax.ShapeDtypeStruct((rows, width), BF16),
                   jax.ShapeDtypeStruct((8, width), F32)],
        cost_estimate=cost(4 * rows * model * width, 67e6),
        compiler_params=params(('arbitrary', 'arbitrary')))(h_two, grad_y, w_fc1, w_fc2, b_fc1)


def run_back(tok_rows, pre_a, pre_b, w1_a, w1_b, x_mid, grad_y, w_out, gain, seq, model):
    batch = tok_rows.shape[0]
    rows, width = pre_a.shape
    group = 2
    tile = group * seq
    vec = jax.ShapeDtypeStruct((8, model), F32)
    vec_spec = pl.BlockSpec((8, model), lambda b: (0, 0))
    row_spec = pl.BlockSpec((tile, model), lambda b: (b, 0))
    return pl.pallas_call(
        back_kernel, grid=(batch // group,), name='back',
        in_specs=[pl.BlockSpec((group, 1, seq), lambda b: (b, 0, 0)),
                  pl.BlockSpec((tile, width), lambda b: (b, 0)), pl.BlockSpec((tile, width), lambda b: (b, 0)),
                  whole((model, width)), whole((model, width)), row_spec, row_spec, out_block(model), whole((1, model))],
        out_specs=[row_spec, row_spec, pl.BlockSpec((group, TAB, model), lambda b: (b, 0, 0)),
                   vec_spec, vec_spec, vec_spec, vec_spec],
        out_shape=[jax.ShapeDtypeStruct((rows, model), BF16), jax.ShapeDtypeStruct((rows, model), BF16),
                   jax.ShapeDtypeStruct((batch, TAB, model), F32), vec, vec, vec, vec],
        cost_estimate=cost(2 * rows * model * (2 * width + model), 90e6),
        compiler_params=params(('arbitrary',)))(
            tok_rows, pre_a, pre_b, w1_a, w1_b, x_mid, grad_y, w_out, gain)


def out_kernel(act_a, act_b, w2_a, w2_b, xmid_ref, bias_ref, out_ref):
    width = 512
    for start in range(0, out_ref.shape[1], width):
        cols = slice(start, start + width)
        total = dot(act_a[...], w2_a[:, :, cols].reshape(-1, width)) + dot(act_b[...], w2_b[:, :, cols].reshape(-1, width))
        out_ref[:, cols] = (xmid_ref[:, cols] + total + bias_ref[:, cols]).astype(BF16)


def run_out(act_a, act_b, w2_a, w2_b, x_mid, b_fc2):
    rows, model = x_mid.shape
    width = act_a.shape[1]
    tile = 512
    weight = pl.BlockSpec((8, 256, model), lambda r: (0, 0, 0), pipeline_mode=pl.Buffered(1))
    act_spec = pl.BlockSpec((tile, width), lambda r: (r, 0))
    row_spec = pl.BlockSpec((tile, model), lambda r: (r, 0))
    return pl.pallas_call(
        out_kernel, grid=(rows // tile,), name='out',
        in_specs=[act_spec, act_spec, weight, weight, row_spec, whole((1, model))],
        out_specs=row_spec, out_shape=jax.ShapeDtypeStruct((rows, model), BF16),
        cost_estimate=cost(4 * rows * model * width, 70e6),
        compiler_params=params(('arbitrary',)))(act_a, act_b, w2_a, w2_b, x_mid, b_fc2)


def solution(mesh):
    row_spec = P(('dp', 'fsdp'), None)
    act_spec = P(('dp', 'fsdp'), None, None)
    param_specs = (P(None, 'fsdp'),) + (P('fsdp'),) * 12
    swap = [(0, 1), (1, 0)]

    def local_step(tokens, grad_y3, *shards):
        (e_part, gain1_part, shift1_part, wqkv_part, bqkv_part, wout_part, bout_part,
         gain2_part, shift2_part, wfc1_part, bfc1_part, wfc2_part, bfc2_part) = shards
        batch, seq = tokens.shape
        vocab = e_part.shape[0]
        model = grad_y3.shape[2]

        def gather(part):
            return lax.all_gather(part, 'fsdp', axis=0, tiled=True)

        smalls = (gain1_part, shift1_part, bout_part, gain2_part, shift2_part, bfc2_part, bqkv_part, bfc1_part)
        packed = jnp.concatenate([e_part] + [part.reshape(-1, 128) for part in smalls], axis=0)
        packed = lax.all_gather(packed, 'fsdp', axis=0, tiled=False)
        w_qkv = gather(wqkv_part)
        joint = lax.all_gather(jnp.concatenate([wfc2_part[:256], wout_part], axis=0), 'fsdp', axis=0, tiled=False)
        wfc1_cut = wfc1_part.reshape(-1, 8, 2, 256)
        w1_a, w1_b = (gather(wfc1_cut[:, :, half].reshape(wfc1_part.shape[0], -1)) for half in range(2))
        w2_b = lax.all_gather(wfc2_part[256:], 'fsdp', axis=0, tiled=False)
        table = packed[:, :vocab].transpose(1, 0, 2).reshape(vocab, model)[:TAB]
        vecs, at = [], vocab
        for part in smalls:
            count = part.shape[0] // 128
            vecs.append(packed[:, at:at + count].reshape(1, -1).astype(F32))
            at += count
        gain1, shift1, b_out, gain2, shift2, b_fc2, b_qkv, b_fc1 = vecs
        grad_y = grad_y3.reshape(batch * seq, model)

        is_mask, is_pad = tokens == MASK_ID, tokens == PAD_ID
        lengths = jnp.sum(jnp.logical_not(is_pad), axis=1).astype(jnp.int32)
        factor = (1.0 - MASK_RATIO) / (1.0 - jnp.sum(is_mask, axis=1).astype(F32) / lengths.astype(F32))
        tok_rows = jnp.where(is_mask, PAD_ID, tokens)[:, None, :]
        keep = jnp.where(jnp.arange(TAB) == PAD_ID, 0.0, factor[:, None])[:, :, None]
        x_tab = (table.astype(F32)[None] * keep).astype(BF16)
        hat_one, inv_one = row_stats(x_tab.astype(F32))
        h_tab = (hat_one * gain1 + shift1).astype(BF16).reshape(batch * TAB, model)
        scale = jnp.where(jnp.arange(3 * model) < model, HEAD_DIM ** -0.5, 1.0)[None]
        qkv_tab = ((dot(h_tab, w_qkv) + b_qkv) * scale).reshape(batch, TAB, 3 * model)

        inv_freq = 1.0 / (ROPE_BASE ** (jnp.arange(0, HEAD_DIM, 2, dtype=F32) / HEAD_DIM))
        angles = inv_freq[:, None] * jnp.arange(seq, dtype=F32)[None, :]
        cos_tab, sin_tab = jnp.cos(angles), jnp.sin(angles)

        qkv_t, ctx, lse = run_attn_fwd(lengths, tok_rows, qkv_tab, cos_tab, sin_tab, seq, model)
        x_mid, h_two = run_mid(tok_rows, ctx, joint, x_tab, b_out, gain2, shift2, seq, model)
        b1_cut = b_fc1.reshape(8, 2, 256)
        b1_a, b1_b = b1_cut[:, 0].reshape(1, -1), b1_cut[:, 1].reshape(1, -1)
        def over_dp(part):
            return part + lax.ppermute(part, 'dp', swap)

        def scatter(grad):
            return lax.psum_scatter(grad, 'fsdp', scatter_dimension=0, tiled=True)

        after = lax.optimization_barrier
        act_a, pre_a, gb1_a = run_mlp(h_two, grad_y, w1_a, joint, b1_a, 'mlp_a')
        raw_fc2a = dot(act_a, grad_y, 0, 0)
        part_fc2a = scatter(raw_fc2a)
        h_two, raw_fc2a = after((h_two, raw_fc2a))
        act_b, pre_b, gb1_b = run_mlp(h_two, grad_y, w1_b, w2_b, b1_b, 'mlp_b')
        pre_a, pre_b, act_b = after((pre_a, pre_b, act_b))
        raw_fc1a = dot(h_two, pre_a, 0, 0)
        part_fc1a = scatter(raw_fc1a)
        act_b, raw_fc1a = after((act_b, raw_fc1a))
        raw_fc2b = dot(act_b, grad_y, 0, 0)
        part_fc2b = scatter(raw_fc2b)
        pre_b, raw_fc2b = after((pre_b, raw_fc2b))
        raw_fc1b = dot(h_two, pre_b, 0, 0)
        part_fc1b = scatter(raw_fc1b)
        pre_a, pre_b, raw_fc1b, part_fc2a = after((pre_a, pre_b, raw_fc1b, part_fc2a))
        d_mid, d_ctx, seg_mid, gg2, gs2, gb_out, gb_fc2 = run_back(
            tok_rows, pre_a, pre_b, w1_a, w1_b, x_mid, grad_y, joint, gain2, seq, model)
        g_fc2a = over_dp(part_fc2a)
        raw_out = dot(ctx, d_mid, 0, 0)
        part_out = scatter(raw_out)
        d_ctx, raw_out, part_fc1a, g_fc2a = after((d_ctx, raw_out, part_fc1a, g_fc2a))
        g_fc1a = over_dp(part_fc1a)
        d_high, d_low, gb_qkv = run_attn_bwd(lengths, tok_rows, qkv_t, lse, d_ctx, cos_tab, sin_tab, seq, model)
        d_high, part_fc2b, part_fc1b, g_fc1a = after((d_high, part_fc2b, part_fc1b, g_fc1a))
        g_fc2b, g_fc1b = over_dp(part_fc2b), over_dp(part_fc1b)
        d_tab = jnp.concatenate([d_high, d_low], axis=0).reshape(2 * batch * TAB, 3 * model)
        raw_qkv = dot(jnp.concatenate([h_tab, h_tab], axis=0), d_tab, 0, 0)
        part_qkv = scatter(raw_qkv)
        d_tab, raw_qkv, act_a, act_b = after((d_tab, raw_qkv, act_a, act_b))
        d_one = dot(d_tab, w_qkv, 1, 1).reshape(2, batch, TAB, model)
        d_one = d_one[0] + d_one[1]
        d_hat = d_one * gain1
        d_x = inv_one * (d_hat - jnp.mean(d_hat, axis=-1, keepdims=True)
                         - hat_one * jnp.mean(d_hat * hat_one, axis=-1, keepdims=True))
        g_table = jnp.sum((seg_mid + d_x) * keep, axis=0)
        g_table = jnp.concatenate([g_table, jnp.zeros((vocab - TAB, model), F32)], axis=0)
        vec_grads = (jnp.sum(d_one * hat_one, axis=(0, 1)), jnp.sum(d_one, axis=(0, 1)), jnp.sum(gb_out, axis=0),
                     jnp.sum(gg2, axis=0), jnp.sum(gs2, axis=0), jnp.sum(gb_fc2, axis=0),
                     jnp.sum(gb_qkv, axis=1),
                     jnp.concatenate([jnp.sum(gb, axis=0).reshape(8, 1, 256) for gb in (gb1_a, gb1_b)], axis=1))
        small = jnp.concatenate(
            [g_table.reshape(vocab, 8, 128).transpose(1, 0, 2)]
            + [vec.reshape(8, -1, 128) for vec in vec_grads], axis=1)
        act_a, act_b, small = after((act_a, act_b, small))
        small = jnp.sum(lax.all_to_all(small, 'fsdp', 0, 0, tiled=True), axis=0)
        hidden = run_out(act_a, act_b, joint, w2_b, x_mid, b_fc2)
        hidden, part_qkv, part_out, small = after((hidden, part_qkv, part_out, small))
        g_w_qkv, g_w_out, small = over_dp(part_qkv), over_dp(part_out), over_dp(small)
        g_small, at = [], vocab
        for part in smalls:
            count = part.shape[0] // 128
            g_small.append(small[at:at + count].reshape(-1))
            at += count
        gg1, gs1, gbo, ggn2, gsh2, gb2, gbq, gb1 = g_small
        hidden = hidden.reshape(grad_y3.shape)
        g_w_fc2 = jnp.concatenate([g_fc2a, g_fc2b], axis=0)
        g_w_fc1 = jnp.concatenate([part.reshape(-1, 8, 1, 256) for part in (g_fc1a, g_fc1b)],
                                  axis=2).reshape(wfc1_part.shape)
        return (hidden, small[:vocab], gg1, gs1, g_w_qkv, gbq, g_w_out, gbo, ggn2, gsh2, g_w_fc1, gb1, g_w_fc2, gb2)

    return jax.shard_map(local_step, mesh=mesh, in_specs=(row_spec, act_spec) + param_specs,
                         out_specs=(act_spec,) + param_specs, check_vma=False)
```

```python
import jax
import jax.numpy as jnp
from jax import lax
from jax.experimental import pallas as pl
from jax.experimental.pallas import tpu as pltpu
from jax.sharding import PartitionSpec as P

HEAD_DIM = 64
HALF = 32
MASK_ID = 32
PAD_ID = 1
TAB = 32
MASK_RATIO = 0.15 * 0.8
LN_EPS = 1e-5
ROPE_BASE = 10000.0
F32 = jnp.float32
BF16 = jnp.bfloat16
NEG = -1e30


def dot(lhs, rhs, lhs_dim=1, rhs_dim=0):
    return lax.dot_general(lhs, rhs, (((lhs_dim,), (rhs_dim,)), ((), ())), preferred_element_type=F32)


def split_two(val):
    high = val.astype(BF16)
    return high, (val - high.astype(F32)).astype(BF16)


def col_sum(val):
    return jnp.sum(val, axis=0, keepdims=True)


def one_hot_t(tok_row, rows):
    index = lax.broadcasted_iota(jnp.int32, (rows, tok_row.shape[1]), 0) & (TAB - 1)
    return jnp.where(index == tok_row, 1.0, 0.0).astype(BF16)


def attn_fwd_kernel(len_ref, tok_ref, tab_ref, cos_ref, sin_ref, qkv_ref, ctx_ref, lse_ref, s_a, s_b, p_a, p_b):
    model = ctx_ref.shape[1]
    seq = ctx_ref.shape[0]
    split = seq // 2
    pairs = model // 128
    length = len_ref[pl.program_id(0)]
    hot = one_hot_t(tok_ref[0], 3 * TAB)
    cos_tab, sin_tab = cos_ref[...], sin_ref[...]
    wide = 256

    def expand(step, carry):
        offset = pl.multiple_of(step * wide, wide)
        part = tab_ref[0, :, pl.ds(offset, wide)]
        high = part.astype(BF16)
        rest = part - high.astype(F32)
        mid = rest.astype(BF16)
        low = (rest - mid.astype(F32)).astype(BF16)
        raw = dot(jnp.concatenate([high, mid, low], axis=0), hot, 0, 0)
        for head in range(wide // HEAD_DIM):
            low_half = raw[head * HEAD_DIM:head * HEAD_DIM + HALF]
            high_half = raw[head * HEAD_DIM + HALF:(head + 1) * HEAD_DIM]
            turned = jnp.concatenate([low_half * cos_tab - high_half * sin_tab,
                                      high_half * cos_tab + low_half * sin_tab], axis=0).astype(BF16)
            qkv_ref[0, pl.ds(pl.multiple_of(offset + head * HEAD_DIM, HEAD_DIM), HEAD_DIM), :] = turned
        return carry

    def expand_v(step, carry):
        offset = pl.multiple_of(2 * model + step * wide, wide)
        part = tab_ref[0, :, pl.ds(offset, wide)].astype(BF16)
        qkv_ref[0, pl.ds(offset, wide), :] = dot(part, hot[:TAB], 0, 0).astype(BF16)
        return carry

    lax.fori_loop(0, 2 * model // wide, expand, 0, unroll=4)
    lax.fori_loop(0, model // wide, expand_v, 0, unroll=4)

    def head_rows(part, step, sub):
        return pl.ds(pl.multiple_of(part * model + step * 128 + sub * HEAD_DIM, HEAD_DIM), HEAD_DIM)

    def score(dst, step):
        for sub in range(2):
            dst[sub] = dot(qkv_ref[0, head_rows(1, step, sub), :], qkv_ref[0, head_rows(0, step, sub), :], 0, 0)

    def soften(src, dst, step):
        key_ok = lax.broadcasted_iota(jnp.int32, (seq - split, seq), 0) + split < length
        for sub in range(2):
            first = src[sub, :split]
            last = jnp.where(key_ok, src[sub, split:], NEG)
            top = jnp.maximum(jnp.max(first, axis=0, keepdims=True), jnp.max(last, axis=0, keepdims=True))
            first, last = jnp.exp(first - top), jnp.exp(last - top)
            total = col_sum(first) + col_sum(last)
            inverse = 1.0 / total
            dst[sub, :split] = (first * inverse).astype(BF16)
            dst[sub, split:] = (last * inverse).astype(BF16)
            lse_ref[0, pl.ds(2 * step + sub, 1), :] = top + jnp.log(total)

    def context(src, step):
        outs = [dot(qkv_ref[0, head_rows(2, step, sub), :], src[sub]) for sub in range(2)]
        ctx_ref[:, pl.ds(pl.multiple_of(step * 128, 128), 128)] = jnp.concatenate(outs, axis=0).T.astype(BF16)

    score(s_a, 0)

    def two_pairs(step, carry):
        even = 2 * step
        score(s_b, even + 1)
        context(p_b, (even + pairs - 1) & (pairs - 1))
        soften(s_a, p_a, even)
        score(s_a, (even + 2) & (pairs - 1))
        context(p_a, even)
        soften(s_b, p_b, even + 1)
        return carry

    lax.fori_loop(0, pairs // 2, two_pairs, 0)
    context(p_b, pairs - 1)


def attn_bwd_kernel(len_ref, tok_ref, q_ref, k_ref, v_ref, lse_ref, dctx_ref, cos_ref, sin_ref, high_ref, low_ref, bias_ref,
                    s_a, s_b, d_a, d_b, p_a, p_b, g_a, g_b, dct):
    model = dctx_ref.shape[1]
    seq = dctx_ref.shape[0]
    split = seq // 2
    pairs = model // 128
    length = len_ref[pl.program_id(0)]
    hot = one_hot_t(tok_ref[0], TAB)
    cos_tab, sin_tab = cos_ref[...], sin_ref[...]

    @pl.when(pl.program_id(0) == 0)
    def _():
        bias_ref[...] = jnp.zeros_like(bias_ref)
        p_b[...] = jnp.zeros_like(p_b)
        g_b[...] = jnp.zeros_like(g_b)

    def flip(step, carry):
        offset = pl.multiple_of(step * 128, 128)
        dct[pl.ds(offset, 128), :] = dctx_ref[:, pl.ds(offset, 128)].T
        return carry

    lax.fori_loop(0, pairs, flip, 0, unroll=4)

    def head_rows(step, sub):
        return pl.ds(pl.multiple_of(step * 128 + sub * HEAD_DIM, HEAD_DIM), HEAD_DIM)

    def unrope(val):
        low, high = val[:HALF], val[HALF:]
        return jnp.concatenate([low * cos_tab + high * sin_tab, high * cos_tab - low * sin_tab], axis=0)

    def put(offset, grad, fresh):
        offset = pl.multiple_of(offset, 128)
        folded = grad[:, :128]
        for lane in range(128, seq, 128):
            folded += grad[:, lane:lane + 128]
        bias_ref[pl.ds(offset, 128), :] += folded * fresh
        sums = dot(hot, grad.astype(BF16), 1, 1)
        high, low = split_two(sums)
        high_ref[0, :, pl.ds(offset, 128)] = high
        low_ref[0, :, pl.ds(offset, 128)] = low

    def score(dst_s, dst_d, step):
        for sub in range(2):
            dst_s[sub] = dot(k_ref[0, head_rows(step, sub), :], q_ref[0, head_rows(step, sub), :], 0, 0)
            dst_d[sub] = dot(v_ref[0, head_rows(step, sub), :], dct[head_rows(step, sub), :], 0, 0)

    def soften(src_s, src_d, dst_p, dst_g, step):
        key_ok = lax.broadcasted_iota(jnp.int32, (seq - split, seq), 0) + split < length
        for sub in range(2):
            lse = lse_ref[0, pl.ds(2 * step + sub, 1), :]
            first = jnp.exp(src_s[sub, :split] - lse)
            last = jnp.exp(jnp.where(key_ok, src_s[sub, split:], NEG) - lse)
            dst_p[sub, :split] = first.astype(BF16)
            dst_p[sub, split:] = last.astype(BF16)
            d_first, d_last = src_d[sub, :split], src_d[sub, split:]
            delta = col_sum(d_first * first) + col_sum(d_last * last)
            dst_g[sub, :split] = (first * (d_first - delta)).astype(BF16)
            dst_g[sub, split:] = (last * (d_last - delta)).astype(BF16)

    def grads(src_p, src_g, step, fresh):
        dq, dk, dv = [], [], []
        for sub in range(2):
            dv.append(dot(dct[head_rows(step, sub), :], src_p[sub], 1, 1))
            dq.append(unrope(dot(k_ref[0, head_rows(step, sub), :], src_g[sub])) * (HEAD_DIM ** -0.5))
            dk.append(unrope(dot(q_ref[0, head_rows(step, sub), :], src_g[sub], 1, 1)))
        put(step * 128, jnp.concatenate(dq, axis=0), fresh)
        put(model + step * 128, jnp.concatenate(dk, axis=0), fresh)
        put(2 * model + step * 128, jnp.concatenate(dv, axis=0), fresh)

    score(s_a, d_a, 0)

    def two_pairs(step, carry):
        even = 2 * step
        score(s_b, d_b, even + 1)
        grads(p_b, g_b, (even + pairs - 1) & (pairs - 1), jnp.where(step == 0, 0.0, 1.0))
        soften(s_a, d_a, p_a, g_a, even)
        score(s_a, d_a, (even + 2) & (pairs - 1))
        grads(p_a, g_a, even, 1.0)
        soften(s_b, d_b, p_b, g_b, even + 1)
        return carry

    lax.fori_loop(0, pairs // 2, two_pairs, 0)
    grads(p_b, g_b, pairs - 1, 1.0)


def fold_rows(val):
    return jnp.sum(val.reshape(val.shape[0] // 8, 8, val.shape[1]), axis=0)


def row_stats(val):
    centered = val - jnp.mean(val, axis=-1, keepdims=True)
    inv_std = lax.rsqrt(jnp.mean(centered * centered, axis=-1, keepdims=True) + LN_EPS)
    return centered * inv_std, inv_std


def flat(ref):
    return ref[...].reshape(-1, ref.shape[-1])


def mid_kernel(tok_ref, ctx_ref, w_ref, tab_ref, bias_ref, gain_ref, shift_ref, xmid_ref, h_ref):
    seq = tok_ref.shape[2]
    for part in range(tok_ref.shape[0]):
        rows = slice(part * seq, (part + 1) * seq)
        hot = one_hot_t(tok_ref[part], TAB)
        x_in = dot(hot, tab_ref[part], 0, 0)
        x_mid = x_in + dot(ctx_ref[rows, :], flat(w_ref)) + bias_ref[...]
        xmid_ref[rows, :] = x_mid
        x_hat, _ = row_stats(x_mid)
        h_ref[rows, :] = (x_hat * gain_ref[...] + shift_ref[...]).astype(BF16)


def mlp_kernel(h_ref, dy_ref, w1_ref, w2_ref, b1_ref, act_ref, dpre_ref, gb_ref):
    width = act_ref.shape[1]
    tile = 256

    @pl.when(pl.program_id(1) == 0)
    def _():
        gb_ref[...] = jnp.zeros_like(gb_ref)

    for start in range(0, width, tile):
        cols = slice(start, start + tile)
        pre = dot(h_ref[...], w1_ref[:, cols]) + b1_ref[:, cols]
        d_act = dot(dy_ref[...], w2_ref[start // tile], 1, 1)
        phi = 0.5 + 0.5 * lax.erf(pre * (2.0 ** -0.5))
        act_ref[:, cols] = (pre * phi).astype(BF16)
        slope = phi + pre * (jnp.exp(pre * pre * -0.5) * 0.3989422804014327)
        d_pre = d_act * slope
        gb_ref[:, cols] += fold_rows(d_pre)
        dpre_ref[:, cols] = d_pre.astype(BF16)


def back_kernel(tok_ref, dpre_a, dpre_b, w1_a, w1_b, xmid_ref, dy_ref, wout_ref, gain_ref,
                dmid_ref, dctx_ref, seg_ref, ggain_ref, gshift_ref, gbout_ref, gbfc2_ref):
    seq = tok_ref.shape[2]

    @pl.when(pl.program_id(0) == 0)
    def _():
        for ref in (ggain_ref, gshift_ref, gbout_ref, gbfc2_ref):
            ref[...] = jnp.zeros_like(ref)

    for part in range(tok_ref.shape[0]):
        rows = slice(part * seq, (part + 1) * seq)
        d_two = dot(dpre_a[rows, :], w1_a[...], 1, 1) + dot(dpre_b[rows, :], w1_b[...], 1, 1)
        x_hat, inv_std = row_stats(xmid_ref[rows, :])
        grad_y = dy_ref[rows, :].astype(F32)
        d_hat = d_two * gain_ref[...]
        d_x = inv_std * (d_hat - jnp.mean(d_hat, axis=-1, keepdims=True)
                         - x_hat * jnp.mean(d_hat * x_hat, axis=-1, keepdims=True))
        d_mid = grad_y + d_x
        ggain_ref[...] += fold_rows(d_two * x_hat)
        gshift_ref[...] += fold_rows(d_two)
        gbout_ref[...] += fold_rows(d_mid)
        gbfc2_ref[...] += fold_rows(grad_y)
        high, low = split_two(d_mid)
        dmid_ref[rows, :] = high
        hot = one_hot_t(tok_ref[part], TAB)
        seg_ref[part] = dot(hot, high) + dot(hot, low)
        dctx_ref[rows, :] = dot(high, flat(wout_ref), 1, 1).astype(BF16)


def whole(shape):
    return pl.BlockSpec(shape, lambda *_: (0,) * len(shape), pipeline_mode=pl.Buffered(1))


def out_block(model):
    return pl.BlockSpec((8, 128, model), lambda *_: (0, 2, 0), pipeline_mode=pl.Buffered(1))


def cost(flops, nbytes):
    return pl.CostEstimate(flops=int(flops), bytes_accessed=int(nbytes), transcendentals=0)


def params(dims):
    return pltpu.CompilerParams(dimension_semantics=dims, vmem_limit_bytes=58720256)


def run_attn_fwd(lengths, tok_rows, tab, cos_tab, sin_tab, seq, model):
    batch = tok_rows.shape[0]
    heads = model // HEAD_DIM
    return pl.pallas_call(
        attn_fwd_kernel, grid=(batch,), name='attn_fwd',
        in_specs=[pl.BlockSpec(memory_space=pltpu.SMEM),
                  pl.BlockSpec((1, 1, seq), lambda b: (b, 0, 0)),
                  pl.BlockSpec((1, TAB, 3 * model), lambda b: (b, 0, 0)),
                  whole((HALF, seq)), whole((HALF, seq))],
        out_specs=[pl.BlockSpec((1, 3 * model, seq), lambda b: (b, 0, 0)),
                   pl.BlockSpec((seq, model), lambda b: (b, 0)),
                   pl.BlockSpec((1, heads, seq), lambda b: (b, 0, 0))],
        out_shape=[jax.ShapeDtypeStruct((batch, 3 * model, seq), BF16),
                   jax.ShapeDtypeStruct((batch * seq, model), BF16),
                   jax.ShapeDtypeStruct((batch, heads, seq), F32)],
        scratch_shapes=[pltpu.VMEM((2, seq, seq), F32)] * 2 + [pltpu.VMEM((2, seq, seq), BF16)] * 2,
        cost_estimate=cost(60e9 * 0.75, 60e6),
        compiler_params=params(('arbitrary',)))(lengths, tok_rows, tab, cos_tab, sin_tab)


def run_attn_bwd(lengths, tok_rows, qkv_t, lse, d_ctx, cos_tab, sin_tab, seq, model, part, parts):
    batch = tok_rows.shape[0]
    width = model // parts
    heads = width // HEAD_DIM

    def slab(kind):
        return pl.BlockSpec((1, width, seq), lambda b: (b, kind * parts + part, 0))

    tab_spec = pl.BlockSpec((1, TAB, 3 * width), lambda b: (b, 0, 0))
    return pl.pallas_call(
        attn_bwd_kernel, grid=(batch,),
        in_specs=[pl.BlockSpec(memory_space=pltpu.SMEM),
                  pl.BlockSpec((1, 1, seq), lambda b: (b, 0, 0)),
                  slab(0), slab(1), slab(2),
                  pl.BlockSpec((1, heads, seq), lambda b: (b, part, 0)),
                  pl.BlockSpec((seq, width), lambda b: (b, part)),
                  whole((HALF, seq)), whole((HALF, seq))],
        out_specs=[tab_spec, tab_spec, pl.BlockSpec((3 * width, 128), lambda b: (0, 0))],
        out_shape=[jax.ShapeDtypeStruct((batch, TAB, 3 * width), BF16),
                   jax.ShapeDtypeStruct((batch, TAB, 3 * width), BF16),
                   jax.ShapeDtypeStruct((3 * width, 128), F32)],
        scratch_shapes=[pltpu.VMEM((2, seq, seq), F32)] * 4 + [pltpu.VMEM((2, seq, seq), BF16)] * 4
        + [pltpu.VMEM((width, seq), BF16)],
        cost_estimate=cost(82e9 / parts, 60e6 / parts),
        compiler_params=params(('arbitrary',)))(
            lengths, tok_rows, qkv_t, qkv_t, qkv_t, lse, d_ctx, cos_tab, sin_tab)


def run_mid(tok_rows, ctx, w_out, x_tab, b_out, gain, shift, seq, model):
    batch = tok_rows.shape[0]
    rows = batch * seq
    group = 2
    tile = group * seq
    return pl.pallas_call(
        mid_kernel, grid=(batch // group,), name='mid',
        in_specs=[pl.BlockSpec((group, 1, seq), lambda b: (b, 0, 0)),
                  pl.BlockSpec((tile, model), lambda b: (b, 0)),
                  out_block(model),
                  pl.BlockSpec((group, TAB, model), lambda b: (b, 0, 0)),
                  whole((1, model)), whole((1, model)), whole((1, model))],
        out_specs=[pl.BlockSpec((tile, model), lambda b: (b, 0)),
                   pl.BlockSpec((tile, model), lambda b: (b, 0))],
        out_shape=[jax.ShapeDtypeStruct((rows, model), F32), jax.ShapeDtypeStruct((rows, model), BF16)],
        cost_estimate=cost(2 * rows * model * model, rows * model * 8),
        compiler_params=params(('arbitrary',)))(tok_rows, ctx, w_out, x_tab, b_out, gain, shift)


def run_mlp(h_two, grad_y, w_fc1, w_fc2, b_fc1):
    rows, model = h_two.shape
    width = w_fc1.shape[1]
    tile, cols = 512, 1024
    return pl.pallas_call(
        mlp_kernel, grid=(width // cols, rows // tile),
        in_specs=[pl.BlockSpec((tile, model), lambda f, r: (r, 0)),
                  pl.BlockSpec((tile, model), lambda f, r: (r, 0)),
                  pl.BlockSpec((model, cols), lambda f, r: (0, f)),
                  pl.BlockSpec((cols // 256, 256, model), lambda f, r: (f, 0, 0)),
                  pl.BlockSpec((1, cols), lambda f, r: (0, f))],
        out_specs=[pl.BlockSpec((tile, cols), lambda f, r: (r, f)),
                   pl.BlockSpec((tile, cols), lambda f, r: (r, f)),
                   pl.BlockSpec((8, cols), lambda f, r: (0, f))],
        out_shape=[jax.ShapeDtypeStruct((rows, width), BF16), jax.ShapeDtypeStruct((rows, width), BF16),
                   jax.ShapeDtypeStruct((8, width), F32)],
        cost_estimate=cost(4 * rows * model * width, 67e6),
        compiler_params=params(('arbitrary', 'arbitrary')))(h_two, grad_y, w_fc1, w_fc2, b_fc1)


def run_back(tok_rows, pre_a, pre_b, w1_a, w1_b, x_mid, grad_y, w_out, gain, seq, model):
    batch = tok_rows.shape[0]
    rows, width = pre_a.shape
    group = 2
    tile = group * seq
    vec = jax.ShapeDtypeStruct((8, model), F32)
    vec_spec = pl.BlockSpec((8, model), lambda b: (0, 0))
    row_spec = pl.BlockSpec((tile, model), lambda b: (b, 0))
    return pl.pallas_call(
        back_kernel, grid=(batch // group,), name='back',
        in_specs=[pl.BlockSpec((group, 1, seq), lambda b: (b, 0, 0)),
                  pl.BlockSpec((tile, width), lambda b: (b, 0)), pl.BlockSpec((tile, width), lambda b: (b, 0)),
                  whole((model, width)), whole((model, width)), row_spec, row_spec, out_block(model), whole((1, model))],
        out_specs=[row_spec, row_spec, pl.BlockSpec((group, TAB, model), lambda b: (b, 0, 0)),
                   vec_spec, vec_spec, vec_spec, vec_spec],
        out_shape=[jax.ShapeDtypeStruct((rows, model), BF16), jax.ShapeDtypeStruct((rows, model), BF16),
                   jax.ShapeDtypeStruct((batch, TAB, model), F32), vec, vec, vec, vec],
        cost_estimate=cost(2 * rows * model * (2 * width + model), 90e6),
        compiler_params=params(('arbitrary',)))(
            tok_rows, pre_a, pre_b, w1_a, w1_b, x_mid, grad_y, w_out, gain)


def out_kernel(act_a, act_b, w2_a, w2_b, xmid_ref, bias_ref, out_ref):
    width = 512
    for start in range(0, out_ref.shape[1], width):
        cols = slice(start, start + width)
        total = dot(act_a[...], w2_a[:, :, cols].reshape(-1, width)) + dot(act_b[...], w2_b[:, :, cols].reshape(-1, width))
        out_ref[:, cols] = (xmid_ref[:, cols] + total + bias_ref[:, cols]).astype(BF16)


def run_out(act_a, act_b, w2_a, w2_b, x_mid, b_fc2):
    rows, model = x_mid.shape
    width = act_a.shape[1]
    tile = 512
    weight = pl.BlockSpec((8, 256, model), lambda r: (0, 0, 0), pipeline_mode=pl.Buffered(1))
    act_spec = pl.BlockSpec((tile, width), lambda r: (r, 0))
    row_spec = pl.BlockSpec((tile, model), lambda r: (r, 0))
    return pl.pallas_call(
        out_kernel, grid=(rows // tile,), name='out',
        in_specs=[act_spec, act_spec, weight, weight, row_spec, whole((1, model))],
        out_specs=row_spec, out_shape=jax.ShapeDtypeStruct((rows, model), BF16),
        cost_estimate=cost(4 * rows * model * width, 70e6),
        compiler_params=params(('arbitrary',)))(act_a, act_b, w2_a, w2_b, x_mid, b_fc2)


def interleave(first, second, width):
    return jnp.concatenate([part[:, at:at + width] for at in range(0, first.shape[1], width)
                            for part in (first, second)], axis=1)


def solution(mesh):
    row_spec = P(('dp', 'fsdp'), None)
    act_spec = P(('dp', 'fsdp'), None, None)
    param_specs = (P(None, 'fsdp'),) + (P('fsdp'),) * 12
    swap = [(0, 1), (1, 0)]

    def local_step(tokens, grad_y3, *shards):
        (e_part, gain1_part, shift1_part, wqkv_part, bqkv_part, wout_part, bout_part,
         gain2_part, shift2_part, wfc1_part, bfc1_part, wfc2_part, bfc2_part) = shards
        batch, seq = tokens.shape
        vocab = e_part.shape[0]
        model = grad_y3.shape[2]

        def gather(part):
            return lax.all_gather(part, 'fsdp', axis=0, tiled=True)

        smalls = (gain1_part, shift1_part, bout_part, gain2_part, shift2_part, bfc2_part, bqkv_part, bfc1_part)
        packed = jnp.concatenate([e_part] + [part.reshape(-1, 128) for part in smalls], axis=0)
        packed = lax.all_gather(packed, 'fsdp', axis=0, tiled=False)
        w_qkv = gather(wqkv_part)
        joint = lax.all_gather(jnp.concatenate([wfc2_part[:256], wout_part], axis=0), 'fsdp', axis=0, tiled=False)
        wfc1_cut = wfc1_part.reshape(-1, 8, 2, 256)
        w1_a, w1_b = (gather(wfc1_cut[:, :, half].reshape(wfc1_part.shape[0], -1)) for half in range(2))
        w2_b = lax.all_gather(wfc2_part[256:], 'fsdp', axis=0, tiled=False)
        table = packed[:, :vocab].transpose(1, 0, 2).reshape(vocab, model)[:TAB]
        vecs, at = [], vocab
        for part in smalls:
            count = part.shape[0] // 128
            vecs.append(packed[:, at:at + count].reshape(1, -1).astype(F32))
            at += count
        gain1, shift1, b_out, gain2, shift2, b_fc2, b_qkv, b_fc1 = vecs
        grad_y = grad_y3.reshape(batch * seq, model)

        is_mask, is_pad = tokens == MASK_ID, tokens == PAD_ID
        lengths = jnp.sum(jnp.logical_not(is_pad), axis=1).astype(jnp.int32)
        factor = (1.0 - MASK_RATIO) / (1.0 - jnp.sum(is_mask, axis=1).astype(F32) / lengths.astype(F32))
        tok_rows = jnp.where(is_mask, PAD_ID, tokens)[:, None, :]
        keep = jnp.where(jnp.arange(TAB) == PAD_ID, 0.0, factor[:, None])[:, :, None]
        x_tab = (table.astype(F32)[None] * keep).astype(BF16)
        hat_one, inv_one = row_stats(x_tab.astype(F32))
        h_tab = (hat_one * gain1 + shift1).astype(BF16).reshape(batch * TAB, model)
        scale = jnp.where(jnp.arange(3 * model) < model, HEAD_DIM ** -0.5, 1.0)[None]
        qkv_tab = ((dot(h_tab, w_qkv) + b_qkv) * scale).reshape(batch, TAB, 3 * model)

        inv_freq = 1.0 / (ROPE_BASE ** (jnp.arange(0, HEAD_DIM, 2, dtype=F32) / HEAD_DIM))
        angles = inv_freq[:, None] * jnp.arange(seq, dtype=F32)[None, :]
        cos_tab, sin_tab = jnp.cos(angles), jnp.sin(angles)

        qkv_t, ctx, lse = run_attn_fwd(lengths, tok_rows, qkv_tab, cos_tab, sin_tab, seq, model)
        x_mid, h_two = run_mid(tok_rows, ctx, joint, x_tab, b_out, gain2, shift2, seq, model)
        b1_cut = b_fc1.reshape(8, 2, 256)
        b1_a, b1_b = b1_cut[:, 0].reshape(1, -1), b1_cut[:, 1].reshape(1, -1)

        def over_dp(part):
            return part + lax.ppermute(part, 'dp', swap)

        def scatter(grad):
            return lax.psum_scatter(grad, 'fsdp', scatter_dimension=0, tiled=True)

        after = lax.optimization_barrier
        act_a, pre_a, gb1_a = run_mlp(h_two, grad_y, w1_a, joint, b1_a)
        raw_fc2a = dot(act_a, grad_y, 0, 0)
        part_fc2a = scatter(raw_fc2a)
        pre_a, raw_fc2a = after((pre_a, raw_fc2a))
        raw_fc1a = dot(h_two, pre_a, 0, 0)
        part_fc1a = scatter(raw_fc1a)
        h_two, raw_fc1a = after((h_two, raw_fc1a))
        act_b, pre_b, gb1_b = run_mlp(h_two, grad_y, w1_b, w2_b, b1_b)
        raw_fc2b = dot(act_b, grad_y, 0, 0)
        part_fc2b = scatter(raw_fc2b)
        pre_b, raw_fc2b = after((pre_b, raw_fc2b))
        raw_fc1b = dot(h_two, pre_b, 0, 0)
        part_fc1b = scatter(raw_fc1b)
        pre_a, pre_b, raw_fc1b, part_fc2a = after((pre_a, pre_b, raw_fc1b, part_fc2a))
        g_fc2a = over_dp(part_fc2a)
        d_mid, d_ctx, seg_mid, gg2, gs2, gb_out, gb_fc2 = run_back(
            tok_rows, pre_a, pre_b, w1_a, w1_b, x_mid, grad_y, joint, gain2, seq, model)
        raw_out = dot(ctx, d_mid, 0, 0)
        part_out = scatter(raw_out)
        d_ctx, raw_out, part_fc1a, g_fc2a = after((d_ctx, raw_out, part_fc1a, g_fc2a))
        g_fc1a = over_dp(part_fc1a)

        def attn_grads(part, d_ctx):
            high, low, bias = run_attn_bwd(
                lengths, tok_rows, qkv_t, lse, d_ctx, cos_tab, sin_tab, seq, model, part, 2)
            return jnp.concatenate([high, low], axis=0).reshape(2 * batch * TAB, -1), bias

        h_pair = jnp.concatenate([h_tab, h_tab], axis=0)
        d_tab0, bias0 = attn_grads(0, d_ctx)
        raw_qkv0 = dot(h_pair, d_tab0, 0, 0)
        part_qkv0 = scatter(raw_qkv0)
        d_ctx, raw_qkv0, part_fc2b, g_fc1a = after((d_ctx, raw_qkv0, part_fc2b, g_fc1a))
        g_fc2b = over_dp(part_fc2b)
        d_tab1, bias1 = attn_grads(1, d_ctx)
        raw_qkv1 = dot(h_pair, d_tab1, 0, 0)
        part_qkv1 = scatter(raw_qkv1)
        d_tab1, raw_qkv1, act_a, act_b, part_fc1b, g_fc2b = after((d_tab1, raw_qkv1, act_a, act_b, part_fc1b, g_fc2b))
        g_fc1b = over_dp(part_fc1b)
        hidden = run_out(act_a, act_b, joint, w2_b, x_mid, b_fc2)
        d_tab1, hidden, g_fc1b, part_out, part_qkv0 = after((d_tab1, hidden, g_fc1b, part_out, part_qkv0))
        g_w_out, g_qkv0 = over_dp(part_out), over_dp(part_qkv0)
        d_tab = interleave(d_tab0, d_tab1, model // 2)
        gb_qkv = jnp.concatenate([jnp.sum(val, axis=1).reshape(3, 1, model // 2) for val in (bias0, bias1)], axis=1)
        d_one = dot(d_tab, w_qkv, 1, 1).reshape(2, batch, TAB, model)
        d_one = d_one[0] + d_one[1]
        d_hat = d_one * gain1
        d_x = inv_one * (d_hat - jnp.mean(d_hat, axis=-1, keepdims=True)
                         - hat_one * jnp.mean(d_hat * hat_one, axis=-1, keepdims=True))
        g_table = jnp.sum((seg_mid + d_x) * keep, axis=0)
        g_table = jnp.concatenate([g_table, jnp.zeros((vocab - TAB, model), F32)], axis=0)
        vec_grads = (jnp.sum(d_one * hat_one, axis=(0, 1)), jnp.sum(d_one, axis=(0, 1)), jnp.sum(gb_out, axis=0),
                     jnp.sum(gg2, axis=0), jnp.sum(gs2, axis=0), jnp.sum(gb_fc2, axis=0),
                     gb_qkv,
                     jnp.concatenate([jnp.sum(gb, axis=0).reshape(8, 1, 256) for gb in (gb1_a, gb1_b)], axis=1))
        small = jnp.concatenate(
            [g_table.reshape(vocab, 8, 128).transpose(1, 0, 2)]
            + [vec.reshape(8, -1, 128) for vec in vec_grads], axis=1)
        small = jnp.sum(lax.all_to_all(small, 'fsdp', 0, 0, tiled=True), axis=0)
        small, g_qkv0, g_w_out = after((small, g_qkv0, g_w_out))
        small = over_dp(small)
        g_qkv1 = over_dp(part_qkv1)
        g_w_qkv = interleave(g_qkv0, g_qkv1, model // 2)
        g_small, at = [], vocab
        for part in smalls:
            count = part.shape[0] // 128
            g_small.append(small[at:at + count].reshape(-1))
            at += count
        gg1, gs1, gbo, ggn2, gsh2, gb2, gbq, gb1 = g_small
        hidden = hidden.reshape(grad_y3.shape)
        g_w_fc2 = jnp.concatenate([g_fc2a, g_fc2b], axis=0)
        g_w_fc1 = jnp.concatenate([part.reshape(-1, 8, 1, 256) for part in (g_fc1a, g_fc1b)],
                                  axis=2).reshape(wfc1_part.shape)
        return (hidden, small[:vocab], gg1, gs1, g_w_qkv, gbq, g_w_out, gbo, ggn2, gsh2, g_w_fc1, gb1, g_w_fc2, gb2)

    return jax.shard_map(local_step, mesh=mesh, in_specs=(row_spec, act_spec) + param_specs,
                         out_specs=(act_spec,) + param_specs, check_vma=False)
```

```python
import jax
import jax.numpy as jnp
from jax import lax
from jax.experimental import pallas as pl
from jax.experimental.pallas import tpu as pltpu
from jax.sharding import PartitionSpec as P

HEAD_DIM = 64
HALF = 32
MASK_ID = 32
PAD_ID = 1
TAB = 32
MASK_RATIO = 0.15 * 0.8
LN_EPS = 1e-5
ROPE_BASE = 10000.0
F32 = jnp.float32
BF16 = jnp.bfloat16
NEG = -1e30


def dot(lhs, rhs, lhs_dim=1, rhs_dim=0):
    return lax.dot_general(lhs, rhs, (((lhs_dim,), (rhs_dim,)), ((), ())), preferred_element_type=F32)


def split_two(val):
    high = val.astype(BF16)
    return high, (val - high.astype(F32)).astype(BF16)


def col_sum(val):
    return jnp.sum(val, axis=0, keepdims=True)


def one_hot_t(tok_row, rows):
    index = lax.broadcasted_iota(jnp.int32, (rows, tok_row.shape[1]), 0) & (TAB - 1)
    return jnp.where(index == tok_row, 1.0, 0.0).astype(BF16)


def attn_fwd_kernel(len_ref, tok_ref, tab_ref, cos_ref, sin_ref, qkv_ref, ctx_ref, lse_ref, s_a, s_b, p_a, p_b):
    model = ctx_ref.shape[1]
    seq = ctx_ref.shape[0]
    split = seq // 2
    pairs = model // 128
    length = len_ref[pl.program_id(0)]
    hot = one_hot_t(tok_ref[0], 3 * TAB)
    cos_tab, sin_tab = cos_ref[...], sin_ref[...]
    wide = 256

    def expand(step, carry):
        offset = pl.multiple_of(step * wide, wide)
        part = tab_ref[0, :, pl.ds(offset, wide)]
        high = part.astype(BF16)
        rest = part - high.astype(F32)
        mid = rest.astype(BF16)
        low = (rest - mid.astype(F32)).astype(BF16)
        raw = dot(jnp.concatenate([high, mid, low], axis=0), hot, 0, 0)
        for head in range(wide // HEAD_DIM):
            low_half = raw[head * HEAD_DIM:head * HEAD_DIM + HALF]
            high_half = raw[head * HEAD_DIM + HALF:(head + 1) * HEAD_DIM]
            turned = jnp.concatenate([low_half * cos_tab - high_half * sin_tab,
                                      high_half * cos_tab + low_half * sin_tab], axis=0).astype(BF16)
            qkv_ref[0, pl.ds(pl.multiple_of(offset + head * HEAD_DIM, HEAD_DIM), HEAD_DIM), :] = turned
        return carry

    def expand_v(step, carry):
        offset = pl.multiple_of(2 * model + step * wide, wide)
        part = tab_ref[0, :, pl.ds(offset, wide)].astype(BF16)
        qkv_ref[0, pl.ds(offset, wide), :] = dot(part, hot[:TAB], 0, 0).astype(BF16)
        return carry

    lax.fori_loop(0, 2 * model // wide, expand, 0, unroll=4)
    lax.fori_loop(0, model // wide, expand_v, 0, unroll=4)

    def head_rows(part, step, sub):
        return pl.ds(pl.multiple_of(part * model + step * 128 + sub * HEAD_DIM, HEAD_DIM), HEAD_DIM)

    def score(dst, step):
        for sub in range(2):
            dst[sub] = dot(qkv_ref[0, head_rows(1, step, sub), :], qkv_ref[0, head_rows(0, step, sub), :], 0, 0)

    def soften(src, dst, step):
        key_ok = lax.broadcasted_iota(jnp.int32, (seq - split, seq), 0) + split < length
        for sub in range(2):
            first = src[sub, :split]
            last = jnp.where(key_ok, src[sub, split:], NEG)
            top = jnp.maximum(jnp.max(first, axis=0, keepdims=True), jnp.max(last, axis=0, keepdims=True))
            first, last = jnp.exp(first - top), jnp.exp(last - top)
            total = col_sum(first) + col_sum(last)
            inverse = 1.0 / total
            dst[sub, :split] = (first * inverse).astype(BF16)
            dst[sub, split:] = (last * inverse).astype(BF16)
            lse_ref[0, pl.ds(2 * step + sub, 1), :] = top + jnp.log(total)

    def context(src, step):
        outs = [dot(qkv_ref[0, head_rows(2, step, sub), :], src[sub]) for sub in range(2)]
        ctx_ref[:, pl.ds(pl.multiple_of(step * 128, 128), 128)] = jnp.concatenate(outs, axis=0).T.astype(BF16)

    score(s_a, 0)

    def two_pairs(step, carry):
        even = 2 * step
        score(s_b, even + 1)
        context(p_b, (even + pairs - 1) & (pairs - 1))
        soften(s_a, p_a, even)
        score(s_a, (even + 2) & (pairs - 1))
        context(p_a, even)
        soften(s_b, p_b, even + 1)
        return carry

    lax.fori_loop(0, pairs // 2, two_pairs, 0)
    context(p_b, pairs - 1)


def attn_bwd_kernel(len_ref, tok_ref, q_ref, k_ref, v_ref, lse_ref, dctx_ref, cos_ref, sin_ref, high_ref, low_ref, bias_ref,
                    s_a, s_b, d_a, d_b, p_a, p_b, g_a, g_b, dct):
    model = dctx_ref.shape[1]
    seq = dctx_ref.shape[0]
    split = seq // 2
    pairs = model // 128
    length = len_ref[pl.program_id(0)]
    hot = one_hot_t(tok_ref[0], TAB)
    cos_tab, sin_tab = cos_ref[...], sin_ref[...]

    @pl.when(pl.program_id(0) == 0)
    def _():
        bias_ref[...] = jnp.zeros_like(bias_ref)
        p_b[...] = jnp.zeros_like(p_b)
        g_b[...] = jnp.zeros_like(g_b)

    def flip(step, carry):
        offset = pl.multiple_of(step * 128, 128)
        dct[pl.ds(offset, 128), :] = dctx_ref[:, pl.ds(offset, 128)].T
        return carry

    lax.fori_loop(0, pairs, flip, 0, unroll=4)

    def head_rows(step, sub):
        return pl.ds(pl.multiple_of(step * 128 + sub * HEAD_DIM, HEAD_DIM), HEAD_DIM)

    def unrope(val):
        low, high = val[:HALF], val[HALF:]
        return jnp.concatenate([low * cos_tab + high * sin_tab, high * cos_tab - low * sin_tab], axis=0)

    def put(offset, grad, fresh):
        offset = pl.multiple_of(offset, 128)
        folded = grad[:, :128]
        for lane in range(128, seq, 128):
            folded += grad[:, lane:lane + 128]
        bias_ref[pl.ds(offset, 128), :] += folded * fresh
        sums = dot(hot, grad.astype(BF16), 1, 1)
        high, low = split_two(sums)
        high_ref[0, :, pl.ds(offset, 128)] = high
        low_ref[0, :, pl.ds(offset, 128)] = low

    def score(dst_s, dst_d, step):
        for sub in range(2):
            dst_s[sub] = dot(k_ref[0, head_rows(step, sub), :], q_ref[0, head_rows(step, sub), :], 0, 0)
            dst_d[sub] = dot(v_ref[0, head_rows(step, sub), :], dct[head_rows(step, sub), :], 0, 0)

    def soften(src_s, src_d, dst_p, dst_g, step):
        key_ok = lax.broadcasted_iota(jnp.int32, (seq - split, seq), 0) + split < length
        for sub in range(2):
            lse = lse_ref[0, pl.ds(2 * step + sub, 1), :]
            first = jnp.exp(src_s[sub, :split] - lse)
            last = jnp.exp(jnp.where(key_ok, src_s[sub, split:], NEG) - lse)
            dst_p[sub, :split] = first.astype(BF16)
            dst_p[sub, split:] = last.astype(BF16)
            d_first, d_last = src_d[sub, :split], src_d[sub, split:]
            delta = col_sum(d_first * first) + col_sum(d_last * last)
            dst_g[sub, :split] = (first * (d_first - delta)).astype(BF16)
            dst_g[sub, split:] = (last * (d_last - delta)).astype(BF16)

    def grads(src_p, src_g, step, fresh):
        dq, dk, dv = [], [], []
        for sub in range(2):
            dv.append(dot(dct[head_rows(step, sub), :], src_p[sub], 1, 1))
            dq.append(unrope(dot(k_ref[0, head_rows(step, sub), :], src_g[sub])) * (HEAD_DIM ** -0.5))
            dk.append(unrope(dot(q_ref[0, head_rows(step, sub), :], src_g[sub], 1, 1)))
        put(step * 128, jnp.concatenate(dq, axis=0), fresh)
        put(model + step * 128, jnp.concatenate(dk, axis=0), fresh)
        put(2 * model + step * 128, jnp.concatenate(dv, axis=0), fresh)

    score(s_a, d_a, 0)

    def two_pairs(step, carry):
        even = 2 * step
        score(s_b, d_b, even + 1)
        grads(p_b, g_b, (even + pairs - 1) & (pairs - 1), jnp.where(step == 0, 0.0, 1.0))
        soften(s_a, d_a, p_a, g_a, even)
        score(s_a, d_a, (even + 2) & (pairs - 1))
        grads(p_a, g_a, even, 1.0)
        soften(s_b, d_b, p_b, g_b, even + 1)
        return carry

    lax.fori_loop(0, pairs // 2, two_pairs, 0)
    grads(p_b, g_b, pairs - 1, 1.0)


def fold_rows(val):
    return jnp.sum(val.reshape(val.shape[0] // 8, 8, val.shape[1]), axis=0)


def row_stats(val):
    centered = val - jnp.mean(val, axis=-1, keepdims=True)
    inv_std = lax.rsqrt(jnp.mean(centered * centered, axis=-1, keepdims=True) + LN_EPS)
    return centered * inv_std, inv_std


def flat(ref):
    return ref[...].reshape(-1, ref.shape[-1])


def mid_kernel(tok_ref, ctx_ref, w_ref, tab_ref, bias_ref, gain_ref, shift_ref, xmid_ref, h_ref):
    seq = tok_ref.shape[2]
    for part in range(tok_ref.shape[0]):
        rows = slice(part * seq, (part + 1) * seq)
        hot = one_hot_t(tok_ref[part], TAB)
        x_in = dot(hot, tab_ref[part], 0, 0)
        x_mid = x_in + dot(ctx_ref[rows, :], flat(w_ref)) + bias_ref[...]
        xmid_ref[rows, :] = x_mid
        x_hat, _ = row_stats(x_mid)
        h_ref[rows, :] = (x_hat * gain_ref[...] + shift_ref[...]).astype(BF16)


def mlp_kernel(h_ref, dy_ref, w1_ref, w2_ref, b1_ref, act_ref, dpre_ref, gb_ref):
    width = act_ref.shape[1]
    tile = 256

    @pl.when(pl.program_id(1) == 0)
    def _():
        gb_ref[...] = jnp.zeros_like(gb_ref)

    for start in range(0, width, tile):
        cols = slice(start, start + tile)
        pre = dot(h_ref[...], w1_ref[:, cols]) + b1_ref[:, cols]
        d_act = dot(dy_ref[...], w2_ref[start // tile], 1, 1)
        phi = 0.5 + 0.5 * lax.erf(pre * (2.0 ** -0.5))
        act_ref[:, cols] = (pre * phi).astype(BF16)
        slope = phi + pre * (jnp.exp(pre * pre * -0.5) * 0.3989422804014327)
        d_pre = d_act * slope
        gb_ref[:, cols] += fold_rows(d_pre)
        dpre_ref[:, cols] = d_pre.astype(BF16)


def back_kernel(tok_ref, dpre_a, dpre_b, w1_a, w1_b, xmid_ref, dy_ref, wout_ref, gain_ref,
                dmid_ref, dctx_ref, seg_ref, ggain_ref, gshift_ref, gbout_ref, gbfc2_ref):
    seq = tok_ref.shape[2]

    @pl.when(pl.program_id(0) == 0)
    def _():
        for ref in (ggain_ref, gshift_ref, gbout_ref, gbfc2_ref):
            ref[...] = jnp.zeros_like(ref)

    for part in range(tok_ref.shape[0]):
        rows = slice(part * seq, (part + 1) * seq)
        d_two = dot(dpre_a[rows, :], w1_a[...], 1, 1) + dot(dpre_b[rows, :], w1_b[...], 1, 1)
        x_hat, inv_std = row_stats(xmid_ref[rows, :])
        grad_y = dy_ref[rows, :].astype(F32)
        d_hat = d_two * gain_ref[...]
        d_x = inv_std * (d_hat - jnp.mean(d_hat, axis=-1, keepdims=True)
                         - x_hat * jnp.mean(d_hat * x_hat, axis=-1, keepdims=True))
        d_mid = grad_y + d_x
        ggain_ref[...] += fold_rows(d_two * x_hat)
        gshift_ref[...] += fold_rows(d_two)
        gbout_ref[...] += fold_rows(d_mid)
        gbfc2_ref[...] += fold_rows(grad_y)
        high, low = split_two(d_mid)
        dmid_ref[rows, :] = high
        hot = one_hot_t(tok_ref[part], TAB)
        seg_ref[part] = dot(hot, high) + dot(hot, low)
        dctx_ref[rows, :] = dot(high, flat(wout_ref), 1, 1).astype(BF16)


def whole(shape):
    return pl.BlockSpec(shape, lambda *_: (0,) * len(shape), pipeline_mode=pl.Buffered(1))


def out_block(model):
    return pl.BlockSpec((8, 128, model), lambda *_: (0, 2, 0), pipeline_mode=pl.Buffered(1))


def cost(flops, nbytes):
    return pl.CostEstimate(flops=int(flops), bytes_accessed=int(nbytes), transcendentals=0)


def params(dims):
    return pltpu.CompilerParams(dimension_semantics=dims, vmem_limit_bytes=58720256)


def run_attn_fwd(lengths, tok_rows, tab, cos_tab, sin_tab, seq, model):
    batch = tok_rows.shape[0]
    heads = model // HEAD_DIM
    return pl.pallas_call(
        attn_fwd_kernel, grid=(batch,), name='attn_fwd',
        in_specs=[pl.BlockSpec(memory_space=pltpu.SMEM),
                  pl.BlockSpec((1, 1, seq), lambda b: (b, 0, 0)),
                  pl.BlockSpec((1, TAB, 3 * model), lambda b: (b, 0, 0)),
                  whole((HALF, seq)), whole((HALF, seq))],
        out_specs=[pl.BlockSpec((1, 3 * model, seq), lambda b: (b, 0, 0)),
                   pl.BlockSpec((seq, model), lambda b: (b, 0)),
                   pl.BlockSpec((1, heads, seq), lambda b: (b, 0, 0))],
        out_shape=[jax.ShapeDtypeStruct((batch, 3 * model, seq), BF16),
                   jax.ShapeDtypeStruct((batch * seq, model), BF16),
                   jax.ShapeDtypeStruct((batch, heads, seq), F32)],
        scratch_shapes=[pltpu.VMEM((2, seq, seq), F32)] * 2 + [pltpu.VMEM((2, seq, seq), BF16)] * 2,
        cost_estimate=cost(60e9 * 0.75, 60e6),
        compiler_params=params(('arbitrary',)))(lengths, tok_rows, tab, cos_tab, sin_tab)


def run_attn_bwd(lengths, tok_rows, qkv_t, lse, d_ctx, cos_tab, sin_tab, seq, model, part, parts):
    batch = tok_rows.shape[0]
    width = model // parts
    heads = width // HEAD_DIM

    def slab(kind):
        return pl.BlockSpec((1, width, seq), lambda b: (b, kind * parts + part, 0))

    tab_spec = pl.BlockSpec((1, TAB, 3 * width), lambda b: (b, 0, 0))
    return pl.pallas_call(
        attn_bwd_kernel, grid=(batch,),
        in_specs=[pl.BlockSpec(memory_space=pltpu.SMEM),
                  pl.BlockSpec((1, 1, seq), lambda b: (b, 0, 0)),
                  slab(0), slab(1), slab(2),
                  pl.BlockSpec((1, heads, seq), lambda b: (b, part, 0)),
                  pl.BlockSpec((seq, width), lambda b: (b, part)),
                  whole((HALF, seq)), whole((HALF, seq))],
        out_specs=[tab_spec, tab_spec, pl.BlockSpec((3 * width, 128), lambda b: (0, 0))],
        out_shape=[jax.ShapeDtypeStruct((batch, TAB, 3 * width), BF16),
                   jax.ShapeDtypeStruct((batch, TAB, 3 * width), BF16),
                   jax.ShapeDtypeStruct((3 * width, 128), F32)],
        scratch_shapes=[pltpu.VMEM((2, seq, seq), F32)] * 4 + [pltpu.VMEM((2, seq, seq), BF16)] * 4
        + [pltpu.VMEM((width, seq), BF16)],
        cost_estimate=cost(82e9 / parts, 60e6 / parts),
        compiler_params=params(('arbitrary',)))(
            lengths, tok_rows, qkv_t, qkv_t, qkv_t, lse, d_ctx, cos_tab, sin_tab)


def run_mid(tok_rows, ctx, w_out, x_tab, b_out, gain, shift, seq, model):
    batch = tok_rows.shape[0]
    rows = batch * seq
    group = 2
    tile = group * seq
    return pl.pallas_call(
        mid_kernel, grid=(batch // group,), name='mid',
        in_specs=[pl.BlockSpec((group, 1, seq), lambda b: (b, 0, 0)),
                  pl.BlockSpec((tile, model), lambda b: (b, 0)),
                  out_block(model),
                  pl.BlockSpec((group, TAB, model), lambda b: (b, 0, 0)),
                  whole((1, model)), whole((1, model)), whole((1, model))],
        out_specs=[pl.BlockSpec((tile, model), lambda b: (b, 0)),
                   pl.BlockSpec((tile, model), lambda b: (b, 0))],
        out_shape=[jax.ShapeDtypeStruct((rows, model), F32), jax.ShapeDtypeStruct((rows, model), BF16)],
        cost_estimate=cost(2 * rows * model * model, rows * model * 8),
        compiler_params=params(('arbitrary',)))(tok_rows, ctx, w_out, x_tab, b_out, gain, shift)


def run_mlp(h_two, grad_y, w_fc1, w_fc2, b_fc1):
    rows, model = h_two.shape
    width = w_fc1.shape[1]
    tile, cols = 512, 1024
    return pl.pallas_call(
        mlp_kernel, grid=(width // cols, rows // tile),
        in_specs=[pl.BlockSpec((tile, model), lambda f, r: (r, 0)),
                  pl.BlockSpec((tile, model), lambda f, r: (r, 0)),
                  pl.BlockSpec((model, cols), lambda f, r: (0, f)),
                  pl.BlockSpec((cols // 256, 256, model), lambda f, r: (f, 0, 0)),
                  pl.BlockSpec((1, cols), lambda f, r: (0, f))],
        out_specs=[pl.BlockSpec((tile, cols), lambda f, r: (r, f)),
                   pl.BlockSpec((tile, cols), lambda f, r: (r, f)),
                   pl.BlockSpec((8, cols), lambda f, r: (0, f))],
        out_shape=[jax.ShapeDtypeStruct((rows, width), BF16), jax.ShapeDtypeStruct((rows, width), BF16),
                   jax.ShapeDtypeStruct((8, width), F32)],
        cost_estimate=cost(4 * rows * model * width, 67e6),
        compiler_params=params(('arbitrary', 'arbitrary')))(h_two, grad_y, w_fc1, w_fc2, b_fc1)


def run_back(tok_rows, pre_a, pre_b, w1_a, w1_b, x_mid, grad_y, w_out, gain, seq, model):
    batch = tok_rows.shape[0]
    rows, width = pre_a.shape
    group = 2
    tile = group * seq
    vec = jax.ShapeDtypeStruct((8, model), F32)
    vec_spec = pl.BlockSpec((8, model), lambda b: (0, 0))
    row_spec = pl.BlockSpec((tile, model), lambda b: (b, 0))
    return pl.pallas_call(
        back_kernel, grid=(batch // group,), name='back',
        in_specs=[pl.BlockSpec((group, 1, seq), lambda b: (b, 0, 0)),
                  pl.BlockSpec((tile, width), lambda b: (b, 0)), pl.BlockSpec((tile, width), lambda b: (b, 0)),
                  whole((model, width)), whole((model, width)), row_spec, row_spec, out_block(model), whole((1, model))],
        out_specs=[row_spec, row_spec, pl.BlockSpec((group, TAB, model), lambda b: (b, 0, 0)),
                   vec_spec, vec_spec, vec_spec, vec_spec],
        out_shape=[jax.ShapeDtypeStruct((rows, model), BF16), jax.ShapeDtypeStruct((rows, model), BF16),
                   jax.ShapeDtypeStruct((batch, TAB, model), F32), vec, vec, vec, vec],
        cost_estimate=cost(2 * rows * model * (2 * width + model), 90e6),
        compiler_params=params(('arbitrary',)))(
            tok_rows, pre_a, pre_b, w1_a, w1_b, x_mid, grad_y, w_out, gain)


def out_kernel(act_a, act_b, w2_a, w2_b, xmid_ref, bias_ref, out_ref):
    width = 512
    for start in range(0, out_ref.shape[1], width):
        cols = slice(start, start + width)
        total = dot(act_a[...], w2_a[:, :, cols].reshape(-1, width)) + dot(act_b[...], w2_b[:, :, cols].reshape(-1, width))
        out_ref[:, cols] = (xmid_ref[:, cols] + total + bias_ref[:, cols]).astype(BF16)


def run_out(act_a, act_b, w2_a, w2_b, x_mid, b_fc2):
    rows, model = x_mid.shape
    width = act_a.shape[1]
    tile = 512
    weight = pl.BlockSpec((8, 256, model), lambda r: (0, 0, 0), pipeline_mode=pl.Buffered(1))
    act_spec = pl.BlockSpec((tile, width), lambda r: (r, 0))
    row_spec = pl.BlockSpec((tile, model), lambda r: (r, 0))
    return pl.pallas_call(
        out_kernel, grid=(rows // tile,), name='out',
        in_specs=[act_spec, act_spec, weight, weight, row_spec, whole((1, model))],
        out_specs=row_spec, out_shape=jax.ShapeDtypeStruct((rows, model), BF16),
        cost_estimate=cost(4 * rows * model * width, 70e6),
        compiler_params=params(('arbitrary',)))(act_a, act_b, w2_a, w2_b, x_mid, b_fc2)


def interleave(first, second, width):
    return jnp.concatenate([part[:, at:at + width] for at in range(0, first.shape[1], width)
                            for part in (first, second)], axis=1)


def solution(mesh):
    row_spec = P(('dp', 'fsdp'), None)
    act_spec = P(('dp', 'fsdp'), None, None)
    param_specs = (P(None, 'fsdp'),) + (P('fsdp'),) * 12
    swap = [(0, 1), (1, 0)]

    def local_step(tokens, grad_y3, *shards):
        (e_part, gain1_part, shift1_part, wqkv_part, bqkv_part, wout_part, bout_part,
         gain2_part, shift2_part, wfc1_part, bfc1_part, wfc2_part, bfc2_part) = shards
        batch, seq = tokens.shape
        vocab = e_part.shape[0]
        model = grad_y3.shape[2]

        def gather(part):
            return lax.all_gather(part, 'fsdp', axis=0, tiled=True)

        smalls = (gain1_part, shift1_part, bout_part, gain2_part, shift2_part, bfc2_part, bqkv_part, bfc1_part)
        packed = jnp.concatenate([e_part] + [part.reshape(-1, 128) for part in smalls], axis=0)
        packed = lax.all_gather(packed, 'fsdp', axis=0, tiled=False)
        w_qkv = gather(wqkv_part)
        joint = lax.all_gather(jnp.concatenate([wfc2_part[:256], wout_part], axis=0), 'fsdp', axis=0, tiled=False)
        wfc1_cut = wfc1_part.reshape(-1, 8, 2, 256)
        w1_a, w1_b = (gather(wfc1_cut[:, :, half].reshape(wfc1_part.shape[0], -1)) for half in range(2))
        w2_b = lax.all_gather(wfc2_part[256:], 'fsdp', axis=0, tiled=False)
        table = packed[:, :vocab].transpose(1, 0, 2).reshape(vocab, model)[:TAB]
        vecs, at = [], vocab
        for part in smalls:
            count = part.shape[0] // 128
            vecs.append(packed[:, at:at + count].reshape(1, -1).astype(F32))
            at += count
        gain1, shift1, b_out, gain2, shift2, b_fc2, b_qkv, b_fc1 = vecs
        grad_y = grad_y3.reshape(batch * seq, model)

        is_mask, is_pad = tokens == MASK_ID, tokens == PAD_ID
        lengths = jnp.sum(jnp.logical_not(is_pad), axis=1).astype(jnp.int32)
        factor = (1.0 - MASK_RATIO) / (1.0 - jnp.sum(is_mask, axis=1).astype(F32) / lengths.astype(F32))
        tok_rows = jnp.where(is_mask, PAD_ID, tokens)[:, None, :]
        keep = jnp.where(jnp.arange(TAB) == PAD_ID, 0.0, factor[:, None])[:, :, None]
        x_tab = (table.astype(F32)[None] * keep).astype(BF16)
        hat_one, inv_one = row_stats(x_tab.astype(F32))
        h_tab = (hat_one * gain1 + shift1).astype(BF16).reshape(batch * TAB, model)
        scale = jnp.where(jnp.arange(3 * model) < model, HEAD_DIM ** -0.5, 1.0)[None]
        qkv_tab = ((dot(h_tab, w_qkv) + b_qkv) * scale).reshape(batch, TAB, 3 * model)

        inv_freq = 1.0 / (ROPE_BASE ** (jnp.arange(0, HEAD_DIM, 2, dtype=F32) / HEAD_DIM))
        angles = inv_freq[:, None] * jnp.arange(seq, dtype=F32)[None, :]
        cos_tab, sin_tab = jnp.cos(angles), jnp.sin(angles)

        qkv_t, ctx, lse = run_attn_fwd(lengths, tok_rows, qkv_tab, cos_tab, sin_tab, seq, model)
        x_mid, h_two = run_mid(tok_rows, ctx, joint, x_tab, b_out, gain2, shift2, seq, model)
        b1_cut = b_fc1.reshape(8, 2, 256)
        b1_a, b1_b = b1_cut[:, 0].reshape(1, -1), b1_cut[:, 1].reshape(1, -1)

        def over_dp(part):
            return part + lax.ppermute(part, 'dp', swap)

        def scatter(grad):
            return lax.psum_scatter(grad, 'fsdp', scatter_dimension=0, tiled=True)

        after = lax.optimization_barrier
        act_a, pre_a, gb1_a = run_mlp(h_two, grad_y, w1_a, joint, b1_a)
        raw_fc2a = dot(act_a, grad_y, 0, 0)
        part_fc2a = scatter(raw_fc2a)
        pre_a, raw_fc2a = after((pre_a, raw_fc2a))
        raw_fc1a = dot(h_two, pre_a, 0, 0)
        part_fc1a = scatter(raw_fc1a)
        h_two, raw_fc1a = after((h_two, raw_fc1a))
        act_b, pre_b, gb1_b = run_mlp(h_two, grad_y, w1_b, w2_b, b1_b)
        raw_fc2b = dot(act_b, grad_y, 0, 0)
        part_fc2b = scatter(raw_fc2b)
        pre_b, raw_fc2b = after((pre_b, raw_fc2b))
        raw_fc1b = dot(h_two, pre_b, 0, 0)
        part_fc1b = scatter(raw_fc1b)
        pre_a, pre_b, raw_fc1b, part_fc2a = after((pre_a, pre_b, raw_fc1b, part_fc2a))
        g_fc2a = over_dp(part_fc2a)
        d_mid, d_ctx, seg_mid, gg2, gs2, gb_out, gb_fc2 = run_back(
            tok_rows, pre_a, pre_b, w1_a, w1_b, x_mid, grad_y, joint, gain2, seq, model)
        raw_out = dot(ctx, d_mid, 0, 0)
        d_ctx, raw_out, part_fc1a, g_fc2a = after((d_ctx, raw_out, part_fc1a, g_fc2a))
        moved_out = lax.all_to_all(raw_out.reshape(8, -1, model), 'fsdp', 0, 0, tiled=True)
        g_fc1a = over_dp(part_fc1a)

        def attn_grads(part, d_ctx):
            high, low, bias = run_attn_bwd(
                lengths, tok_rows, qkv_t, lse, d_ctx, cos_tab, sin_tab, seq, model, part, 2)
            return jnp.concatenate([high, low], axis=0).reshape(2 * batch * TAB, -1), bias

        h_pair = jnp.concatenate([h_tab, h_tab], axis=0)
        d_tab0, bias0 = attn_grads(0, d_ctx)
        raw_qkv0 = dot(h_pair, d_tab0, 0, 0)
        part_qkv0 = scatter(raw_qkv0)
        d_ctx, raw_qkv0, part_fc2b, g_fc1a, moved_out = after((d_ctx, raw_qkv0, part_fc2b, g_fc1a, moved_out))
        part_out = jnp.sum(moved_out, axis=0)
        g_fc2b = over_dp(part_fc2b)
        d_tab1, bias1 = attn_grads(1, d_ctx)
        raw_qkv1 = dot(h_pair, d_tab1, 0, 0)
        part_qkv1 = scatter(raw_qkv1)
        d_tab1, raw_qkv1, act_a, act_b, part_fc1b, g_fc2b = after((d_tab1, raw_qkv1, act_a, act_b, part_fc1b, g_fc2b))
        g_fc1b = over_dp(part_fc1b)
        hidden = run_out(act_a, act_b, joint, w2_b, x_mid, b_fc2)
        d_tab1, hidden, g_fc1b, part_out, part_qkv0 = after((d_tab1, hidden, g_fc1b, part_out, part_qkv0))
        g_w_out, g_qkv0 = over_dp(part_out), over_dp(part_qkv0)
        d_tab = interleave(d_tab0, d_tab1, model // 2)
        gb_qkv = jnp.concatenate([jnp.sum(val, axis=1).reshape(3, 1, model // 2) for val in (bias0, bias1)], axis=1)
        d_one = dot(d_tab, w_qkv, 1, 1).reshape(2, batch, TAB, model)
        d_one = d_one[0] + d_one[1]
        d_hat = d_one * gain1
        d_x = inv_one * (d_hat - jnp.mean(d_hat, axis=-1, keepdims=True)
                         - hat_one * jnp.mean(d_hat * hat_one, axis=-1, keepdims=True))
        g_table = jnp.sum((seg_mid + d_x) * keep, axis=0)
        g_table = jnp.concatenate([g_table, jnp.zeros((vocab - TAB, model), F32)], axis=0)
        vec_grads = (jnp.sum(d_one * hat_one, axis=(0, 1)), jnp.sum(d_one, axis=(0, 1)), jnp.sum(gb_out, axis=0),
                     jnp.sum(gg2, axis=0), jnp.sum(gs2, axis=0), jnp.sum(gb_fc2, axis=0),
                     gb_qkv,
                     jnp.concatenate([jnp.sum(gb, axis=0).reshape(8, 1, 256) for gb in (gb1_a, gb1_b)], axis=1))
        small = jnp.concatenate(
            [g_table.reshape(vocab, 8, 128).transpose(1, 0, 2)]
            + [vec.reshape(8, -1, 128) for vec in vec_grads], axis=1)
        small = jnp.sum(lax.all_to_all(small, 'fsdp', 0, 0, tiled=True), axis=0)
        small, g_qkv0, g_w_out = after((small, g_qkv0, g_w_out))
        small = over_dp(small)
        g_qkv1 = over_dp(part_qkv1)
        g_w_qkv = interleave(g_qkv0, g_qkv1, model // 2)
        g_small, at = [], vocab
        for part in smalls:
            count = part.shape[0] // 128
            g_small.append(small[at:at + count].reshape(-1))
            at += count
        gg1, gs1, gbo, ggn2, gsh2, gb2, gbq, gb1 = g_small
        hidden = hidden.reshape(grad_y3.shape)
        g_w_fc2 = jnp.concatenate([g_fc2a, g_fc2b], axis=0)
        g_w_fc1 = jnp.concatenate([part.reshape(-1, 8, 1, 256) for part in (g_fc1a, g_fc1b)],
                                  axis=2).reshape(wfc1_part.shape)
        return (hidden, small[:vocab], gg1, gs1, g_w_qkv, gbq, g_w_out, gbo, ggn2, gsh2, g_w_fc1, gb1, g_w_fc2, gb2)

    return jax.shard_map(local_step, mesh=mesh, in_specs=(row_spec, act_spec) + param_specs,
                         out_specs=(act_spec,) + param_specs, check_vma=False)
```
